32 devices in a mesh: dp: 8 (over z, x), sub: 4 (over y, core).
Axes of the slice: x: 2, y: 2, z: 4, core: 2. Of those that a mesh axis runs over, the one named last changes fastest.
Arguments:
- block_in: bfloat16 [32, 322, 1152], P(('dp', 'sub')), may hold values from -6 to 6
- long_skip: bfloat16 [32, 322, 1152], P(('dp', 'sub')), may hold values from -6 to 6
- lengths: int32 [32], P(('dp', 'sub')), may hold values from 192 to 320, as said below
- grad_out: bfloat16 [32, 322, 1152], P(('dp', 'sub')), may hold values from -6 to 6
- w_skip: bfloat16 [2654208], P(('dp', 'sub')), may hold values from -0.125 to 0.125
- w_qkv: bfloat16 [3981312], P(('dp', 'sub')), may hold values from -0.1875 to 0.1875
- w_out: bfloat16 [1327104], P(('dp', 'sub')), may hold values from -1.5 to 1.5
- w_up: bfloat16 [5308416], P(('dp', 'sub')), may hold values from -0.1875 to 0.1875
- w_down: bfloat16 [5308416], P(('dp', 'sub')), may hold values from -0.09375 to 0.09375
- norm_gains: float32 [2, 1152], replicated, may hold values from 0.5 to 1.5
- biases: float32 [9, 1152], replicated, may hold values from -3 to 3
Outputs:
- layer_out: bfloat16 [32, 322, 1152], P(('dp', 'sub'))
- grad_in: bfloat16 [32, 322, 1152], P(('dp', 'sub'))
- grad_skip: bfloat16 [32, 322, 1152], P(('dp', 'sub'))
- grad_w_skip: float32 [2654208], P(('dp', 'sub'))
- grad_w_qkv: float32 [3981312], P(('dp', 'sub'))
- grad_w_out: float32 [1327104], P(('dp', 'sub'))
- grad_w_up: float32 [5308416], P(('dp', 'sub'))
- grad_w_down: float32 [5308416], P(('dp', 'sub'))
- grad_gains: float32 [2, 1152], replicated
- grad_biases: float32 [9, 1152], replicated
The draws below stay inside these ranges and needn't reach their ends.
Inputs may be any that keep to these rules, and one draw needn't show every extreme that they name: In each item, slots 0 and 1 hold its time and class tokens, slots 2 to lengths + 1 hold its patches, and the rest is padding; in every draw at least one item has 320 patches and one has 192.
All inputs are finite; a program needn't handle non-finite values.
Results may differ from the reference program's by a relative error of at most 0.014.
Values may be sent and summed in bfloat16 or wider, within the bound.
A program may use at most 320 MiB of HBM per device.

```python
import jax
import jax.numpy as jnp
from jax import lax

D = 1152
HEADS = 16
HD = 72
FF = 4608
PATCH_MAX = 320
PATCH_MIN = 192
ITEMS_DEV = 1
SLOTS = 322
N_ITEMS = 32


def draw_lengths(key, part):
    first_key, second_key = jax.random.split(jax.random.fold_in(key, 17))
    drawn = jax.random.randint(first_key, (N_ITEMS,), PATCH_MIN, PATCH_MAX + 1)
    places = jax.random.permutation(second_key, N_ITEMS)
    drawn = drawn.at[places[0]].set(PATCH_MAX)
    drawn = drawn.at[places[1]].set(PATCH_MIN)
    return drawn.astype(jnp.int32)


def shard_levels(rng, shape, shards, low, top_value):
    def one(dim, shards_of):
        steps = jax.random.uniform(jax.random.fold_in(jax.random.fold_in(rng, 6), dim), (shards_of,), jnp.float32, low / len(shards), top_value / len(shards))
        return jnp.repeat(jnp.exp(steps), shape[dim] // shards_of).reshape((-1,) + (1,) * (len(shape) - dim - 1))

    level = one(*shards[0])
    for cut in shards[1:]:
        level = level * one(*cut)
    return level


def normal_values(own_key, extent, scale, limit, cuts=(), kind=jnp.bfloat16):
    values = scale * jax.random.normal(own_key, extent, jnp.float32)
    if cuts:
        values = values * shard_levels(own_key, extent, cuts, -0.22, 0.18)
    return jnp.clip(values, -limit, limit).astype(kind)


def setup_inputs(seed: int = 0) -> dict:
    seeds = jax.random.split(jax.random.key(seed), 12)
    return {
        "block_in": normal_values(seeds[0], (N_ITEMS, SLOTS, D), 1.0, 6.0, ((0, 32),)),
        "long_skip": normal_values(seeds[1], (N_ITEMS, SLOTS, D), 1.0, 6.0, ((0, 32),)),
        "lengths": draw_lengths(jax.random.fold_in(seeds[11], 71), 0),
        "grad_out": normal_values(seeds[3], (N_ITEMS, SLOTS, D), 1.0, 6.0, ((0, 32),)),
        "w_skip": normal_values(seeds[4], (2 * D * D,), (2 * D) ** -0.5, 0.125, ((0, 32),)),
        "w_qkv": normal_values(seeds[5], (3 * D * D,), D ** -0.5, 0.1875, ((0, 32),)),
        "w_out": normal_values(seeds[6], (D * D,), (D // 64) ** -0.5, 1.5, ((0, 32),)),
        "w_up": normal_values(seeds[7], (D * FF,), D ** -0.5, 0.1875, ((0, 32),)),
        "w_down": normal_values(seeds[8], (FF * D,), FF ** -0.5, 0.09375, ((0, 32),)),
        "norm_gains": jnp.clip(1.0 + 0.1 * jax.random.normal(seeds[9], (2, D), jnp.float32), 0.5, 1.5),
        "biases": normal_values(seeds[10], (9, D), 0.5, 3.0, (), jnp.float32),
    }


@jax.custom_vjp
def low(v):
    return lax.optimization_barrier(v.astype(jnp.bfloat16)).astype(jnp.float32)

@jax.custom_vjp
def low_back(v):
    return v

def low_keep(v):
    return (low(v), None)

def low_pass(kept, grad):
    return (grad,)

def back_keep(v):
    return (v, None)

def back_low(kept, grad):
    return (low(grad),)
low.defvjp(low_keep, low_pass)
low_back.defvjp(back_keep, back_low)
norm_epsilon = 1e-05
masked_score = -1e+30

def precise(left_side, right_side):
    return jnp.dot(left_side, right_side, precision=lax.Precision.HIGHEST, preferred_element_type=jnp.float32)

def layer_norm(stream, gain_row, shift_row):
    centred = stream - lax.optimization_barrier(jnp.mean(stream, -1, keepdims=True))
    inverse = lax.rsqrt(lax.optimization_barrier(jnp.mean(centred * centred, -1, keepdims=True)) + norm_epsilon)
    return centred * inverse * gain_row + shift_row

def forward(block_rows, skip_rows, params, key_valid):
    w_skip, w_qkv, w_out, w_up, w_down, gain_rows, shift_rows = params
    item_count = block_rows.shape[0]
    row_count = item_count * SLOTS
    joined = jnp.concatenate([block_rows, skip_rows], -1).reshape(row_count, 2 * D)
    stream_one = low_back(precise(joined, w_skip) + shift_rows[0])
    normed = low(layer_norm(stream_one, gain_rows[0], shift_rows[1]))
    triple = low_back(low(precise(normed, w_qkv))).reshape(item_count, SLOTS, 3, HEADS, HD)
    queries = triple[:, :, 0]
    key_rows = triple[:, :, 1]
    values = triple[:, :, 2]
    scores = jnp.einsum('ishd,ithd->ihst', queries, key_rows, precision=lax.Precision.HIGHEST) * HD ** (-0.5)
    scores = low_back(scores)
    scores = jnp.where(key_valid[:, None, None, :], scores, masked_score)
    highest = lax.optimization_barrier(jnp.max(scores, -1, keepdims=True))
    raised = jnp.exp(scores - highest)
    shares = low(raised / lax.optimization_barrier(jnp.sum(raised, -1, keepdims=True)))
    mixture = jnp.einsum('ihst,ithd->ishd', shares, values, precision=lax.Precision.HIGHEST)
    mixture = low_back(low(mixture.reshape(row_count, D)))
    stream_two = stream_one + low_back(precise(mixture, w_out) + shift_rows[2])
    normed_two = low(layer_norm(stream_two, gain_rows[1], shift_rows[3]))
    hidden = low_back(precise(normed_two, w_up) + shift_rows[4:8].reshape(FF))
    active = low(jax.nn.gelu(hidden, approximate=False))
    result = stream_two + low_back(precise(active, w_down) + shift_rows[8])
    return result.reshape(item_count, SLOTS, D)

def widen(array):
    return array.astype(jnp.float32)

def reference(block_in, long_skip, lengths, grad_out, w_skip, w_qkv, w_out, w_up, w_down, norm_gains, biases):
    params = (widen(w_skip).reshape(2 * D, D), widen(w_qkv).reshape(D, 3 * D), widen(w_out).reshape(D, D), widen(w_up).reshape(D, FF), widen(w_down).reshape(FF, D), widen(norm_gains), widen(biases))
    group_size = 4 * ITEMS_DEV
    group_count = N_ITEMS // group_size

    def regroup(array):
        return array.reshape((group_count, group_size) + array.shape[1:])
    positions = jnp.arange(SLOTS, dtype=jnp.int32)

    def scan_step(totals, batched):
        inputs, skips, sizes, cotangent = batched
        key_valid = positions[None, :] < sizes[:, None] + 2

        def forward_group(block_rows, skip_rows, weights):
            return forward(block_rows, skip_rows, weights, key_valid)
        outputs, pullback = jax.vjp(forward_group, widen(inputs), widen(skips), params)
        start_grad = widen(cotangent) * key_valid[:, :, None].astype(jnp.float32)
        grad_block, grad_long, grad_params = pullback(start_grad)

        def accumulate(total, grad):
            return total + grad
        totals = jax.tree.map(accumulate, totals, grad_params)
        return (totals, (outputs.astype(jnp.bfloat16), grad_block.astype(jnp.bfloat16), grad_long.astype(jnp.bfloat16)))
    zeros = jax.tree.map(jnp.zeros_like, params)
    totals, (outputs, grad_block, grad_long) = lax.scan(scan_step, zeros, (regroup(block_in), regroup(long_skip), regroup(lengths), regroup(grad_out)))
    layer_out = outputs.reshape(N_ITEMS, SLOTS, D)
    grad_in = grad_block.reshape(N_ITEMS, SLOTS, D)
    grad_skip = grad_long.reshape(N_ITEMS, SLOTS, D)
    return (layer_out, grad_in, grad_skip, totals[0].reshape(-1), totals[1].reshape(-1), totals[2].reshape(-1), totals[3].reshape(-1), totals[4].reshape(-1), totals[5], totals[6])
```

```python
import functools

import jax
import jax.numpy as jnp
from jax import lax
from jax.sharding import PartitionSpec as P


HEADS = 16
HD = 72
FF = 4608


norm_epsilon = 1e-05
masked_score = -1e30


def product(left_side, right_side):
    return jnp.dot(left_side, right_side, preferred_element_type=jnp.float32)


def cross_rows(left_side, right_side):
    return lax.dot_general(
        left_side, right_side, (((0,), (0,)), ((), ())), preferred_element_type=jnp.float32
    )


def cross_cols(left_side, right_side):
    return lax.dot_general(
        left_side, right_side, (((1,), (1,)), ((), ())), preferred_element_type=jnp.float32
    )


FLAT_AXES = ("dp", "sub")
GATHER_X_LAST = (3, 4, 1, 2, 0)
GATHER_Y_LAST = (3, 4, 2, 1, 0)


def bit_order(device_count, wanted):
    bits = device_count.bit_length() - 1
    return wanted if bits == len(wanted) else tuple(range(bits))


def swap_with(array, bit, device_count):
    pairs = [(place, place ^ (1 << bit)) for place in range(device_count)]
    return lax.ppermute(array, FLAT_AXES, pairs)


def own_bit(bit):
    return (lax.axis_index(FLAT_AXES) >> bit) & 1


def can_halve(row_count, device_count):
    return device_count & (device_count - 1) == 0 and row_count % device_count == 0


def gather_rows(flat_shard, row_count, column_count, device_count, wanted):
    if not can_halve(row_count, device_count):
        whole = lax.all_gather(flat_shard, FLAT_AXES, axis=0, tiled=True)
        return whole.reshape(row_count, column_count)
    shard_rows = row_count // device_count
    held = flat_shard.reshape(1, shard_rows, column_count)
    done = []
    for bit in bit_order(device_count, wanted):
        other = swap_with(held, bit, device_count)
        low = sum(1 for place in done if place < bit)
        shape = (-1, 1, 2**low, shard_rows, column_count)
        first = own_bit(bit) == 0
        mine, theirs = held.reshape(shape), other.reshape(shape)
        held = jnp.concatenate(
            [jnp.where(first, mine, theirs), jnp.where(first, theirs, mine)], 1
        )
        held = held.reshape(-1, shard_rows, column_count)
        done.append(bit)
    return held.reshape(row_count, column_count)


def scatter_rows(block, device_count, wanted):
    row_count, column_count = block.shape
    if not can_halve(row_count, device_count):
        return lax.psum_scatter(
            block.reshape(-1), FLAT_AXES, scatter_dimension=0, tiled=True
        )
    shard_rows = row_count // device_count
    held = block.astype(jnp.bfloat16).reshape(device_count, shard_rows, column_count)
    left = set(range(device_count.bit_length() - 1))
    for bit in reversed(bit_order(device_count, wanted)):
        left.remove(bit)
        low = sum(1 for place in left if place < bit)
        shape = (-1, 2, 2**low * shard_rows, column_count)
        halves = held.reshape(shape)
        mine = own_bit(bit)
        sent = lax.dynamic_index_in_dim(halves, 1 - mine, 1, keepdims=False)
        kept = lax.dynamic_index_in_dim(halves, mine, 1, keepdims=False)
        got = swap_with(sent, bit, device_count)
        total = kept.astype(jnp.float32) + got.astype(jnp.float32)
        held = total.astype(jnp.bfloat16) if left else total
    return held.reshape(-1)


def sum_everywhere(block, device_count):
    if device_count & (device_count - 1):
        return lax.psum(block, FLAT_AXES)
    for bit in range(device_count.bit_length() - 1):
        block = block + swap_with(block, bit, device_count)
    return block


def norm_forward(stream, gain_row, shift_row):
    centred = stream - jnp.mean(stream, -1, keepdims=True)
    inverse = lax.rsqrt(jnp.mean(centred * centred, -1, keepdims=True) + norm_epsilon)
    normal = centred * inverse
    return (normal * gain_row + shift_row, normal, inverse)


def norm_backward(incoming, normal, inverse, gain_row):
    grad_gain = jnp.sum(incoming * normal, 0)
    grad_shift = jnp.sum(incoming, 0)
    scaled = incoming * gain_row
    centred = scaled - jnp.mean(scaled, -1, keepdims=True)
    grad_value = inverse * (centred - normal * jnp.mean(scaled * normal, -1, keepdims=True))
    return (grad_value, grad_gain, grad_shift)


def gelu_slope(hidden):
    cumulative = 0.5 * (1.0 + lax.erf(hidden * 0.5**0.5))
    density = jnp.exp(-0.5 * hidden * hidden) * (2.0 * jnp.pi) ** (-0.5)
    return cumulative + hidden * density


def attention_shares(queries, key_rows, key_valid, score_scale):
    scores = (
        jnp.einsum("ishd,ithd->ihst", queries, key_rows, preferred_element_type=jnp.float32)
        * score_scale
    )
    scores = jnp.where(key_valid[:, None, None, :], scores, masked_score)
    highest = jnp.max(scores, -1, keepdims=True)
    raised = jnp.exp(scores - highest)
    return raised / jnp.sum(raised, -1, keepdims=True)


def on_device(
    device_count,
    block_in,
    long_skip,
    lengths,
    grad_out,
    w_skip,
    w_qkv,
    w_out,
    w_up,
    w_down,
    norm_gains,
    biases,
):
    item_count, slot_count, model_width = block_in.shape
    row_count = item_count * slot_count
    head_count = HEADS
    head_size = HD
    hidden_width = FF
    score_scale = HD ** (-0.5)
    key_valid = jnp.arange(slot_count, dtype=jnp.int32)[None, :] < lengths[:, None] + 2
    skip_full = gather_rows(
        w_skip, 2 * model_width, model_width, device_count, GATHER_X_LAST
    )
    qkv_full = gather_rows(
        w_qkv, model_width, 3 * model_width, device_count, GATHER_Y_LAST
    )
    out_full = gather_rows(w_out, model_width, model_width, device_count, GATHER_X_LAST)
    up_full = gather_rows(w_up, model_width, hidden_width, device_count, GATHER_Y_LAST)
    down_full = gather_rows(w_down, hidden_width, model_width, device_count, GATHER_X_LAST)
    joined = jnp.concatenate([block_in, long_skip], -1).reshape(row_count, 2 * model_width)
    stream_one = product(joined, skip_full) + biases[0]
    normed, normal_one, inverse_one = norm_forward(stream_one, norm_gains[0], biases[1])
    normed_low = normed.astype(jnp.bfloat16)
    triple = product(normed_low, qkv_full).astype(jnp.bfloat16)
    triple = triple.reshape(item_count, slot_count, 3, head_count, head_size)
    queries = triple[:, :, 0]
    key_rows = triple[:, :, 1]
    values = triple[:, :, 2]
    shares = attention_shares(queries, key_rows, key_valid, score_scale)
    shares_low = shares.astype(jnp.bfloat16)
    mixture = jnp.einsum("ihst,ithd->ishd", shares_low, values, preferred_element_type=jnp.float32)
    mixture_low = mixture.reshape(row_count, model_width).astype(jnp.bfloat16)
    stream_two = stream_one + (product(mixture_low, out_full) + biases[2])
    normed_two, normal_two, inverse_two = norm_forward(stream_two, norm_gains[1], biases[3])
    normed_two_low = normed_two.astype(jnp.bfloat16)
    hidden = product(normed_two_low, up_full) + biases[4:8].reshape(hidden_width)
    active_low = jax.nn.gelu(hidden, approximate=False).astype(jnp.bfloat16)
    result = stream_two + (product(active_low, down_full) + biases[8])
    layer_out = result.astype(jnp.bfloat16).reshape(item_count, slot_count, model_width)
    row_mask = key_valid.reshape(row_count, 1).astype(jnp.float32)
    start_grad = grad_out.reshape(row_count, model_width).astype(jnp.float32) * row_mask
    grad_branch = start_grad.astype(jnp.bfloat16)
    bias_down = jnp.sum(grad_branch.astype(jnp.float32), 0)
    part_down = scatter_rows(
        cross_rows(active_low, grad_branch), device_count, GATHER_X_LAST
    )
    grad_active = cross_cols(grad_branch, down_full)
    grad_hidden = (grad_active * gelu_slope(hidden)).astype(jnp.bfloat16)
    bias_up = jnp.sum(grad_hidden.astype(jnp.float32), 0)
    part_up = scatter_rows(
        cross_rows(normed_two_low, grad_hidden), device_count, GATHER_Y_LAST
    )
    grad_normed_two = cross_cols(grad_hidden, up_full)
    local_two, gain_two, shift_two = norm_backward(
        grad_normed_two, normal_two, inverse_two, norm_gains[1]
    )
    grad_two = start_grad + local_two
    grad_attn = grad_two.astype(jnp.bfloat16)
    bias_out = jnp.sum(grad_attn.astype(jnp.float32), 0)
    part_out = scatter_rows(
        cross_rows(mixture_low, grad_attn), device_count, GATHER_X_LAST
    )
    grad_mixture = cross_cols(grad_attn, out_full).astype(jnp.bfloat16)
    grad_mixture = grad_mixture.reshape(item_count, slot_count, head_count, head_size)
    grad_shares = jnp.einsum(
        "ishd,ithd->ihst", grad_mixture, values, preferred_element_type=jnp.float32
    )
    grad_scores = shares * (grad_shares - jnp.sum(shares * grad_shares, -1, keepdims=True))
    grad_scores_low = grad_scores.astype(jnp.bfloat16)
    grad_queries = (
        jnp.einsum("ihst,ithd->ishd", grad_scores_low, key_rows, preferred_element_type=jnp.float32)
        * score_scale
    )
    grad_keys = (
        jnp.einsum("ihst,ishd->ithd", grad_scores_low, queries, preferred_element_type=jnp.float32)
        * score_scale
    )
    grad_values = jnp.einsum(
        "ihst,ishd->ithd", shares_low, grad_mixture, preferred_element_type=jnp.float32
    )
    grad_triple = jnp.stack([grad_queries, grad_keys, grad_values], 2).astype(jnp.bfloat16)
    grad_triple = grad_triple.reshape(row_count, 3 * model_width)
    part_qkv = scatter_rows(
        cross_rows(normed_low, grad_triple), device_count, GATHER_Y_LAST
    )
    grad_normed = cross_cols(grad_triple, qkv_full)
    local_one, gain_one, shift_one = norm_backward(
        grad_normed, normal_one, inverse_one, norm_gains[0]
    )
    grad_one = (grad_two + local_one).astype(jnp.bfloat16)
    bias_skip = jnp.sum(grad_one.astype(jnp.float32), 0)
    part_skip = scatter_rows(
        cross_rows(joined, grad_one), device_count, GATHER_X_LAST
    )
    grad_joined = cross_cols(grad_one, skip_full).reshape(item_count, slot_count, 2 * model_width)
    grad_in = grad_joined[:, :, :model_width].astype(jnp.bfloat16)
    grad_skip = grad_joined[:, :, model_width:].astype(jnp.bfloat16)
    gains_part = jnp.stack([gain_one, gain_two], 0)
    biases_part = jnp.concatenate(
        [
            jnp.stack([bias_skip, shift_one, bias_out, shift_two], 0),
            bias_up.reshape(4, model_width),
            bias_down[None, :],
        ],
        0,
    )
    small_sums = sum_everywhere(jnp.concatenate([gains_part, biases_part], 0), device_count)
    grad_gains, grad_biases = small_sums[:2], small_sums[2:]
    return (
        layer_out,
        grad_in,
        grad_skip,
        part_skip,
        part_qkv,
        part_out,
        part_up,
        part_down,
        grad_gains,
        grad_biases,
    )


def solution(mesh):
    placed = (
        P(("dp", "sub"), None, None),
        P(("dp", "sub"), None, None),
        P(("dp", "sub")),
        P(("dp", "sub"), None, None),
        P(("dp", "sub")),
        P(("dp", "sub")),
        P(("dp", "sub")),
        P(("dp", "sub")),
        P(("dp", "sub")),
        P(),
        P(),
    )
    device_count = mesh.shape["dp"] * mesh.shape["sub"]
    return jax.shard_map(
        functools.partial(on_device, device_count),
        mesh=mesh,
        in_specs=placed,
        out_specs=(
            P(("dp", "sub"), None, None),
            P(("dp", "sub"), None, None),
            P(("dp", "sub"), None, None),
            P(("dp", "sub")),
            P(("dp", "sub")),
            P(("dp", "sub")),
            P(("dp", "sub")),
            P(("dp", "sub")),
            P(),
            P(),
        ),
        check_vma=False,
    )
```

```python
import functools

import jax
import jax.numpy as jnp
from jax import lax
from jax.experimental import pallas as pl
from jax.experimental.pallas import tpu as pltpu
from jax.sharding import PartitionSpec as P


HEADS = 16
HD = 72
FF = 4608


norm_epsilon = 1e-05
masked_score = -1e30


def product(left_side, right_side):
    return jnp.dot(left_side, right_side, preferred_element_type=jnp.float32)


def cross_rows(left_side, right_side):
    return lax.dot_general(
        left_side, right_side, (((0,), (0,)), ((), ())), preferred_element_type=jnp.float32
    )


def cross_cols(left_side, right_side):
    return lax.dot_general(
        left_side, right_side, (((1,), (1,)), ((), ())), preferred_element_type=jnp.float32
    )


FLAT_AXES = ("dp", "sub")
GATHER_X_LAST = (3, 4, 1, 2, 0)
GATHER_Y_LAST = (3, 4, 2, 1, 0)


def bit_order(device_count, wanted):
    bits = device_count.bit_length() - 1
    return wanted if bits == len(wanted) else tuple(range(bits))


def swap_with(array, bit, device_count):
    pairs = [(place, place ^ (1 << bit)) for place in range(device_count)]
    return lax.ppermute(array, FLAT_AXES, pairs)


def own_bit(bit):
    return (lax.axis_index(FLAT_AXES) >> bit) & 1


def can_halve(row_count, device_count):
    return device_count & (device_count - 1) == 0 and row_count % device_count == 0


def gather_rows(flat_shard, row_count, column_count, device_count, wanted):
    if not can_halve(row_count, device_count):
        whole = lax.all_gather(flat_shard, FLAT_AXES, axis=0, tiled=True)
        return whole.reshape(row_count, column_count)
    shard_rows = row_count // device_count
    held = flat_shard.reshape(1, shard_rows, column_count)
    done = []
    for bit in bit_order(device_count, wanted):
        other = swap_with(held, bit, device_count)
        low = sum(1 for place in done if place < bit)
        shape = (-1, 1, 2**low, shard_rows, column_count)
        first = own_bit(bit) == 0
        mine, theirs = held.reshape(shape), other.reshape(shape)
        held = jnp.concatenate(
            [jnp.where(first, mine, theirs), jnp.where(first, theirs, mine)], 1
        )
        held = held.reshape(-1, shard_rows, column_count)
        done.append(bit)
    return held.reshape(row_count, column_count)


def scatter_rows(block, device_count, wanted):
    row_count, column_count = block.shape
    if not can_halve(row_count, device_count):
        return lax.psum_scatter(
            block.reshape(-1), FLAT_AXES, scatter_dimension=0, tiled=True
        )
    shard_rows = row_count // device_count
    held = block.astype(jnp.bfloat16).reshape(device_count, shard_rows, column_count)
    left = set(range(device_count.bit_length() - 1))
    for bit in reversed(bit_order(device_count, wanted)):
        left.remove(bit)
        low = sum(1 for place in left if place < bit)
        shape = (-1, 2, 2**low * shard_rows, column_count)
        halves = held.reshape(shape)
        mine = own_bit(bit)
        sent = lax.dynamic_index_in_dim(halves, 1 - mine, 1, keepdims=False)
        kept = lax.dynamic_index_in_dim(halves, mine, 1, keepdims=False)
        got = swap_with(sent, bit, device_count)
        total = kept.astype(jnp.float32) + got.astype(jnp.float32)
        held = total.astype(jnp.bfloat16) if left else total
    return held.reshape(-1)


def sum_everywhere(block, device_count):
    if device_count & (device_count - 1):
        return lax.psum(block, FLAT_AXES)
    for bit in range(device_count.bit_length() - 1):
        block = block + swap_with(block, bit, device_count)
    return block


MESH_IDS = pl.DeviceIdType.MESH


def place_of():
    spread, near = lax.axis_index("dp"), lax.axis_index("sub")
    return spread // 2, spread % 2, near // 2, near % 2


def device_at(place):
    z, x, y, core = place
    return (z * 2 + x, y * 2 + core)


def partner_of(place, step):
    z, x, y, core = place
    if step == "z1":
        return (z + 1 - 2 * (z % 2), x, y, core)
    if step == "z2":
        return (z + 2 - 4 * (z // 2), x, y, core)
    if step == "x":
        return (z, 1 - x, y, core)
    if step == "y":
        return (z, x, 1 - y, core)
    return (z, x, y, 1 - core)


ALL_STEPS = ("z1", "z2", "x", "y", "core")


def greet_partners(place):
    barrier = pltpu.get_barrier_semaphore()
    for step in ALL_STEPS:
        pl.semaphore_signal(
            barrier,
            inc=1,
            device_id=device_at(partner_of(place, step)),
            device_id_type=MESH_IDS,
        )
    pl.semaphore_wait(barrier, len(ALL_STEPS))


def held_region(whole, place, step, last):
    z, x, y, core = place
    if step == "z1":
        return whole.at[z, x, y]
    if step == "z2":
        return whole.at[pl.ds(2 * (z // 2), 2), x, y]
    if step == "core":
        return whole
    if step != last:
        return whole.at[:, x, y]
    if step == "x":
        return whole.at[:, x]
    return whole.at[:, :, y]


SKIP, QKV, OUT, UP, DOWN = range(5)
PIECES = (
    (QKV, "columns", 4, 0, 23, 4, 0, 23, "y"),
    (OUT, "columns", 5, 0, 4, 4, 0, 5, "x"),
    (QKV, "columns", 5, 9, 13, 4, 9, 14, "y"),
    (SKIP, "rows", 48, 0, 0, 48, 0, 0, "x"),
    (QKV, "columns", 5, 4, 18, 5, 4, 18, "y"),
    (SKIP, "rows", 24, 48, 48, 24, 48, 48, "x"),
    (UP, "columns", 6, 0, 18, 6, 0, 18, "y"),
    (DOWN, "rows", 48, 0, 0, 48, 0, 0, "x"),
    (UP, "columns", 6, 6, 24, 6, 6, 24, "y"),
    (DOWN, "rows", 48, 48, 48, 48, 48, 48, "x"),
    (UP, "columns", 6, 12, 30, 6, 12, 30, "y"),
    (DOWN, "rows", 48, 96, 96, 48, 96, 96, "x"),
)
PIECE_GROUPS = (0, 0, 1, 1, 2, 2, 3, 3, 4, 4, 5, 5)
GROUP_COUNT = 6
PIECE_COUNT = len(PIECES)
WINDOW_FIRST = {QKV: (0, 13), OUT: (0, 4), UP: (0, 18)}


def piece_columns(size, first_zero, first_one, owner):
    first = 128 * (first_zero + owner * (first_one - first_zero))
    return pl.ds(pl.multiple_of(first, 128), 128 * size)


def piece_window(whole, piece, owner):
    _, axis, size, first_zero, first_one = piece[:5]
    if axis == "rows":
        return whole.at[:, :, :, owner, pl.ds(first_zero, size)]
    return whole.at[:, :, :, :, piece_columns(size, first_zero, first_one, owner)]


def gather_kernel(
    skip_in, qkv_in, out_in, up_in, down_in,
    skip_out, qkv_out, out_out, up_out, down_out,
    local_sems, send_sems, recv_sems,
):
    place = place_of()
    core = place[3]
    sources = (skip_in, qkv_in, out_in, up_in, down_in)
    targets = (skip_out, qkv_out, out_out, up_out, down_out)
    items = []
    for piece in PIECES:
        weight, axis, size, first_zero, first_one = piece[:5]
        window = piece_window(targets[weight], piece, core)
        if axis == "rows":
            source, passed = sources[weight].at[pl.ds(first_zero, size)], window
        else:
            source = sources[weight].at[:, piece_columns(size, first_zero, first_one, core)]
            passed = targets[weight].at[:, :, :, :, piece_columns(*piece[5:8], core)]
        items.append((source, window, passed, piece[8]))

    def local_copy(index):
        source, whole, _, _ = items[index]
        z, x, y, _ = place
        return pltpu.make_async_copy(source, whole.at[z, x, y], local_sems.at[index])

    def remote_copy(index, phase):
        source, whole, passed, last = items[index]
        steps = ("z1", "z2") + (("x", "y") if last == "y" else ("y", "x")) + ("core",)
        step = steps[phase]
        target = held_region(passed if step == "core" else whole, place, step, last)
        return pltpu.make_async_remote_copy(
            src_ref=source if phase == 0 else target,
            dst_ref=target,
            send_sem=send_sems.at[index, phase],
            recv_sem=recv_sems.at[index, phase],
            device_id=device_at(partner_of(place, step)),
            device_id_type=MESH_IDS,
        )

    for index in range(len(items)):
        local_copy(index).start()
    greet_partners(place)
    for slot in range(GROUP_COUNT + 4):
        for phase, index in (
            (phase, index)
            for phase in (0, 1, 3, 2, 4)
            for index in range(PIECE_COUNT)
            if PIECE_GROUPS[index] == slot - phase
        ):
            if phase == 1:
                local_copy(index).wait()
            if phase > 0:
                remote_copy(index, phase - 1).wait_recv()
            remote_copy(index, phase).start()
    for index in range(len(items)):
        remote_copy(index, 4).wait_recv()
    for index in range(len(items)):
        for phase in range(5):
            remote_copy(index, phase).wait_send()


def join_core_pair(shard, device_count):
    other = swap_with(shard, 0, device_count)
    first = own_bit(0) == 0
    return jnp.concatenate(
        [jnp.where(first, shard, other), jnp.where(first, other, shard)], 0
    )


def gather_weights(w_skip, w_qkv, w_out, w_up, w_down, model_width, hidden_width, device_count):
    sources = (
        w_skip.reshape(-1, model_width),
        join_core_pair(w_qkv.reshape(-1, 3 * model_width), device_count),
        join_core_pair(w_out.reshape(-1, model_width), device_count),
        join_core_pair(w_up.reshape(-1, hidden_width), device_count),
        w_down.reshape(-1, model_width),
    )
    leads = ((4, 2, 2, 2), (4, 2, 2), (4, 2, 2), (4, 2, 2), (4, 2, 2, 2))
    wholes = pl.pallas_call(
        gather_kernel,
        out_shape=[
            jax.ShapeDtypeStruct(lead + source.shape, source.dtype)
            for lead, source in zip(leads, sources)
        ],
        in_specs=[pl.BlockSpec(memory_space=pltpu.VMEM)] * 5,
        out_specs=[pl.BlockSpec(memory_space=pl.ANY)] * 5,
        scratch_shapes=[
            pltpu.SemaphoreType.DMA((PIECE_COUNT,)),
            pltpu.SemaphoreType.DMA((PIECE_COUNT, 5)),
            pltpu.SemaphoreType.DMA((PIECE_COUNT, 5)),
        ],
        compiler_params=pltpu.CompilerParams(collective_id=0, has_side_effects=True),
        name="gather_weights",
    )(*sources)
    return tuple(whole.reshape(-1, whole.shape[-1]) for whole in wholes)


def tuned_mesh(mesh_sizes, model_width, hidden_width):
    return mesh_sizes == (8, 4) and (model_width, hidden_width) == (1152, 4608)


SCATTER_GROUPS = tuple(GROUP_COUNT - 1 - group for group in PIECE_GROUPS)
SCATTER_SHAPES = tuple(
    (piece[2], 1152) if piece[1] == "rows" else (72, 128 * piece[2]) for piece in PIECES
)
RESULT_SHAPES = ((72, 1152), (72, 1792), (72, 640), (72, 2304), (144, 1152))
SMALL_ROWS = 16


def scatter_kernel(
    skip_grad, qkv_grad, out_grad, up_grad, down_grad, small_in, *rest
):
    item_count = len(SCATTER_SHAPES)
    results, rest = rest[:5], rest[5:]
    small_out, rest = rest[0], rest[1:]
    sums, rest = rest[:item_count], rest[item_count:]
    arrived, rest = rest[: 5 * item_count], rest[5 * item_count :]
    small_held, small_arrived, local_sems, send_sems, recv_sems, small_send, small_recv = rest
    place = place_of()
    z, x, y, core = place
    other_core = 1 - core

    grads = (skip_grad, qkv_grad, out_grad, up_grad, down_grad)

    def source(index, owner):
        return piece_window(grads[PIECES[index][0]], PIECES[index], owner)

    def result_window(index):
        weight, axis, size, first_zero, first_one = PIECES[index][:5]
        if axis == "rows":
            return results[weight].at[pl.ds(first_zero, size)]
        low, high = WINDOW_FIRST[weight]
        spot = piece_columns(size, first_zero - low, first_one - high, core)
        return results[weight].at[:, spot]

    def steps_of(index):
        middle = ("y", "x") if PIECES[index][8] == "y" else ("x", "y")
        return ("core",) + middle + ("z2", "z1")

    def sent_region(index, phase):
        held = sums[index]
        step = steps_of(index)[phase]
        if step == "core":
            return source(index, other_core)
        if step == "z2":
            return held.at[pl.ds(2 - 2 * (z // 2), 2), x, y]
        if step == "z1":
            return held.at[z + 1 - 2 * (z % 2), x, y]
        if step == "x":
            return held.at[:, 1 - x] if phase == 1 else held.at[:, 1 - x, y]
        return held.at[:, :, 1 - y] if phase == 1 else held.at[:, x, 1 - y]

    def local_copy(index):
        return pltpu.make_async_copy(
            source(index, core), sums[index], local_sems.at[index]
        )

    def remote_copy(index, phase):
        return pltpu.make_async_remote_copy(
            src_ref=sent_region(index, phase),
            dst_ref=arrived[5 * index + phase],
            send_sem=send_sems.at[index, phase],
            recv_sem=recv_sems.at[index, phase],
            device_id=device_at(partner_of(place, steps_of(index)[phase])),
            device_id_type=MESH_IDS,
        )

    def small_copy(phase):
        return pltpu.make_async_remote_copy(
            src_ref=small_held.at[phase],
            dst_ref=small_arrived.at[phase],
            send_sem=small_send.at[phase],
            recv_sem=small_recv.at[phase],
            device_id=device_at(partner_of(place, ALL_STEPS[phase])),
            device_id_type=MESH_IDS,
        )

    def add_arrived(index, phase):
        held, got = sums[index], arrived[5 * index + phase]
        step = steps_of(index)[phase]

        def total(mine, theirs):
            return mine.astype(jnp.float32) + theirs.astype(jnp.float32)

        if step == "z1":
            result_window(index)[...] = total(held[z, x, y], got[...])
            return

        def one(turn, carry):
            if step == "core":
                spot = (turn // 4, (turn // 2) % 2, turn % 2)
                taken = got[turn // 4, (turn // 2) % 2, turn % 2]
            elif step == "z2":
                spot, taken = (2 * (z // 2) + turn, x, y), got[turn]
            elif phase == 2:
                spot, taken = (turn, x, y), got[turn]
            elif step == "x":
                spot, taken = (turn // 2, x, turn % 2), got[turn // 2, turn % 2]
            else:
                spot, taken = (turn // 2, turn % 2, y), got[turn // 2, turn % 2]
            held[spot] = total(held[spot], taken).astype(jnp.bfloat16)
            return carry

        lax.fori_loop(0, (16, 8, 4, 2)[phase], one, 0)

    for index in reversed(range(item_count)):
        local_copy(index).start()
    small_held[0] = small_in[...]
    greet_partners(place)
    for index in reversed(range(item_count)):
        remote_copy(index, 0).start()
    small_copy(0).start()
    for slot in range(GROUP_COUNT + 4):
        for index in range(item_count):
            phase = slot - SCATTER_GROUPS[index]
            if phase < 0 or phase > 4:
                continue
            if phase == 0:
                local_copy(index).wait()
            remote_copy(index, phase).wait_recv()
            add_arrived(index, phase)
            if phase < 4:
                remote_copy(index, phase + 1).start()
        if slot < 5:
            small_copy(slot).wait_recv()
            summed = small_held[slot] + small_arrived[slot]
            if slot < 4:
                small_held[slot + 1] = summed
                small_copy(slot + 1).start()
            else:
                small_out[...] = summed
    for phase in range(5):
        small_copy(phase).wait_send()
        for index in range(item_count):
            remote_copy(index, phase).wait_send()


def split_core_pair(window, row_count, column_count, passed, device_count):
    core = own_bit(0)
    kept_rows = lax.dynamic_slice_in_dim(window, core * row_count, row_count, 0)
    sent_rows = lax.dynamic_slice_in_dim(window, (1 - core) * row_count, row_count, 0)
    got = swap_with(sent_rows, 0, device_count)
    first = core == 0
    left = jnp.concatenate([kept_rows, got[:, got.shape[1] - passed :]], 1)
    right = jnp.concatenate([got[:, :passed], kept_rows], 1)
    return jnp.where(first, left, right).reshape(-1)


def scatter_gradients(skip_grad, qkv_grad, out_grad, up_grad, down_grad, small, device_count):
    blocks = [
        block.astype(jnp.bfloat16).reshape(lead + (-1, block.shape[-1]))
        for block, lead in (
            (skip_grad, (4, 2, 2, 2)),
            (qkv_grad, (4, 2, 2)),
            (out_grad, (4, 2, 2)),
            (up_grad, (4, 2, 2)),
            (down_grad, (4, 2, 2, 2)),
        )
    ]
    small_count, width = small.shape
    padded = jnp.pad(small, ((0, SMALL_ROWS - small_count), (0, 0)))
    leads = ((4, 2, 2), (4, 2), (4,), (2,), ())
    item_count = len(SCATTER_SHAPES)
    outcome = pl.pallas_call(
        scatter_kernel,
        out_shape=[jax.ShapeDtypeStruct(shape, jnp.float32) for shape in RESULT_SHAPES]
        + [jax.ShapeDtypeStruct((SMALL_ROWS, width), jnp.float32)],
        in_specs=[pl.BlockSpec(memory_space=pl.ANY)] * 5
        + [pl.BlockSpec(memory_space=pltpu.VMEM)],
        out_specs=[pl.BlockSpec(memory_space=pltpu.VMEM)] * 6,
        scratch_shapes=[
            pltpu.VMEM((4, 2, 2) + shape, jnp.bfloat16) for shape in SCATTER_SHAPES
        ]
        + [
            pltpu.VMEM(lead + shape, jnp.bfloat16)
            for shape in SCATTER_SHAPES
            for lead in leads
        ]
        + [
            pltpu.VMEM((5, SMALL_ROWS, width), jnp.float32),
            pltpu.VMEM((5, SMALL_ROWS, width), jnp.float32),
            pltpu.SemaphoreType.DMA((item_count,)),
            pltpu.SemaphoreType.DMA((item_count, 5)),
            pltpu.SemaphoreType.DMA((item_count, 5)),
            pltpu.SemaphoreType.DMA((5,)),
            pltpu.SemaphoreType.DMA((5,)),
        ],
        compiler_params=pltpu.CompilerParams(
            collective_id=1, has_side_effects=True, vmem_limit_bytes=66_000_000
        ),
        name="scatter_gradients",
    )(*blocks, padded)
    skip_part, qkv_part, out_part, up_part, down_part, summed = outcome
    part_up = split_core_pair(up_part, 36, 4608, 2304, device_count)
    part_qkv = split_core_pair(qkv_part, 36, 3456, 1664, device_count)
    part_out = split_core_pair(out_part, 36, 1152, 512, device_count)
    part_down = down_part.reshape(-1)
    return (
        skip_part.reshape(-1), part_qkv, part_out, part_up, part_down, summed[:small_count]
    )


def norm_forward(stream, gain_row, shift_row):
    centred = stream - jnp.mean(stream, -1, keepdims=True)
    inverse = lax.rsqrt(jnp.mean(centred * centred, -1, keepdims=True) + norm_epsilon)
    normal = centred * inverse
    return (normal * gain_row + shift_row, normal, inverse)


def norm_backward(incoming, normal, inverse, gain_row):
    grad_gain = jnp.sum(incoming * normal, 0)
    grad_shift = jnp.sum(incoming, 0)
    scaled = incoming * gain_row
    centred = scaled - jnp.mean(scaled, -1, keepdims=True)
    grad_value = inverse * (centred - normal * jnp.mean(scaled * normal, -1, keepdims=True))
    return (grad_value, grad_gain, grad_shift)


def gelu_slope(hidden):
    cumulative = 0.5 * (1.0 + lax.erf(hidden * 0.5**0.5))
    density = jnp.exp(-0.5 * hidden * hidden) * (2.0 * jnp.pi) ** (-0.5)
    return cumulative + hidden * density


def attention_shares(queries, key_rows, key_valid, score_scale):
    scores = (
        jnp.einsum("ishd,ithd->ihst", queries, key_rows, preferred_element_type=jnp.float32)
        * score_scale
    )
    scores = jnp.where(key_valid[:, None, None, :], scores, masked_score)
    highest = jnp.max(scores, -1, keepdims=True)
    raised = jnp.exp(scores - highest)
    return raised / jnp.sum(raised, -1, keepdims=True)


def on_device(
    mesh_sizes,
    block_in,
    long_skip,
    lengths,
    grad_out,
    w_skip,
    w_qkv,
    w_out,
    w_up,
    w_down,
    norm_gains,
    biases,
):
    item_count, slot_count, model_width = block_in.shape
    device_count = mesh_sizes[0] * mesh_sizes[1]
    row_count = item_count * slot_count
    head_count = HEADS
    head_size = HD
    hidden_width = FF
    score_scale = HD ** (-0.5)
    key_valid = jnp.arange(slot_count, dtype=jnp.int32)[None, :] < lengths[:, None] + 2
    if tuned_mesh(mesh_sizes, model_width, hidden_width):
        skip_full, qkv_full, out_full, up_full, down_full = gather_weights(
            w_skip, w_qkv, w_out, w_up, w_down, model_width, hidden_width, device_count
        )
    else:
        skip_full = gather_rows(
            w_skip, 2 * model_width, model_width, device_count, GATHER_X_LAST
        )
        qkv_full = gather_rows(
            w_qkv, model_width, 3 * model_width, device_count, GATHER_Y_LAST
        )
        out_full = gather_rows(w_out, model_width, model_width, device_count, GATHER_X_LAST)
        up_full = gather_rows(w_up, model_width, hidden_width, device_count, GATHER_Y_LAST)
        down_full = gather_rows(w_down, hidden_width, model_width, device_count, GATHER_X_LAST)
    joined = jnp.concatenate([block_in, long_skip], -1).reshape(row_count, 2 * model_width)
    stream_one = product(joined, skip_full) + biases[0]
    normed, normal_one, inverse_one = norm_forward(stream_one, norm_gains[0], biases[1])
    normed_low = normed.astype(jnp.bfloat16)
    triple = product(normed_low, qkv_full).astype(jnp.bfloat16)
    triple = triple.reshape(item_count, slot_count, 3, head_count, head_size)
    queries = triple[:, :, 0]
    key_rows = triple[:, :, 1]
    values = triple[:, :, 2]
    shares = attention_shares(queries, key_rows, key_valid, score_scale)
    shares_low = shares.astype(jnp.bfloat16)
    mixture = jnp.einsum("ihst,ithd->ishd", shares_low, values, preferred_element_type=jnp.float32)
    mixture_low = mixture.reshape(row_count, model_width).astype(jnp.bfloat16)
    stream_two = stream_one + (product(mixture_low, out_full) + biases[2])
    normed_two, normal_two, inverse_two = norm_forward(stream_two, norm_gains[1], biases[3])
    normed_two_low = normed_two.astype(jnp.bfloat16)
    hidden = product(normed_two_low, up_full) + biases[4:8].reshape(hidden_width)
    active_low = jax.nn.gelu(hidden, approximate=False).astype(jnp.bfloat16)
    result = stream_two + (product(active_low, down_full) + biases[8])
    layer_out = result.astype(jnp.bfloat16).reshape(item_count, slot_count, model_width)
    row_mask = key_valid.reshape(row_count, 1).astype(jnp.float32)
    start_grad = grad_out.reshape(row_count, model_width).astype(jnp.float32) * row_mask
    grad_branch = start_grad.astype(jnp.bfloat16)
    bias_down = jnp.sum(grad_branch.astype(jnp.float32), 0)
    block_down = cross_rows(active_low, grad_branch)
    grad_active = cross_cols(grad_branch, down_full)
    grad_hidden = (grad_active * gelu_slope(hidden)).astype(jnp.bfloat16)
    bias_up = jnp.sum(grad_hidden.astype(jnp.float32), 0)
    block_up = cross_rows(normed_two_low, grad_hidden)
    grad_normed_two = cross_cols(grad_hidden, up_full)
    local_two, gain_two, shift_two = norm_backward(
        grad_normed_two, normal_two, inverse_two, norm_gains[1]
    )
    grad_two = start_grad + local_two
    grad_attn = grad_two.astype(jnp.bfloat16)
    bias_out = jnp.sum(grad_attn.astype(jnp.float32), 0)
    block_out = cross_rows(mixture_low, grad_attn)
    grad_mixture = cross_cols(grad_attn, out_full).astype(jnp.bfloat16)
    grad_mixture = grad_mixture.reshape(item_count, slot_count, head_count, head_size)
    grad_shares = jnp.einsum(
        "ishd,ithd->ihst", grad_mixture, values, preferred_element_type=jnp.float32
    )
    grad_scores = shares * (grad_shares - jnp.sum(shares * grad_shares, -1, keepdims=True))
    grad_scores_low = grad_scores.astype(jnp.bfloat16)
    grad_queries = (
        jnp.einsum("ihst,ithd->ishd", grad_scores_low, key_rows, preferred_element_type=jnp.float32)
        * score_scale
    )
    grad_keys = (
        jnp.einsum("ihst,ishd->ithd", grad_scores_low, queries, preferred_element_type=jnp.float32)
        * score_scale
    )
    grad_values = jnp.einsum(
        "ihst,ishd->ithd", shares_low, grad_mixture, preferred_element_type=jnp.float32
    )
    grad_triple = jnp.stack([grad_queries, grad_keys, grad_values], 2).astype(jnp.bfloat16)
    grad_triple = grad_triple.reshape(row_count, 3 * model_width)
    block_qkv = cross_rows(normed_low, grad_triple)
    grad_normed = cross_cols(grad_triple, qkv_full)
    local_one, gain_one, shift_one = norm_backward(
        grad_normed, normal_one, inverse_one, norm_gains[0]
    )
    grad_one = (grad_two + local_one).astype(jnp.bfloat16)
    bias_skip = jnp.sum(grad_one.astype(jnp.float32), 0)
    block_skip = cross_rows(joined, grad_one)
    grad_joined = cross_cols(grad_one, skip_full).reshape(item_count, slot_count, 2 * model_width)
    grad_in = grad_joined[:, :, :model_width].astype(jnp.bfloat16)
    grad_skip = grad_joined[:, :, model_width:].astype(jnp.bfloat16)
    gains_part = jnp.stack([gain_one, gain_two], 0)
    biases_part = jnp.concatenate(
        [
            jnp.stack([bias_skip, shift_one, bias_out, shift_two], 0),
            bias_up.reshape(4, model_width),
            bias_down[None, :],
        ],
        0,
    )
    small = jnp.concatenate([gains_part, biases_part], 0)
    if tuned_mesh(mesh_sizes, model_width, hidden_width):
        part_skip, part_qkv, part_out, part_up, part_down, small_sums = scatter_gradients(
            block_skip, block_qkv, block_out, block_up, block_down, small, device_count
        )
    else:
        part_skip = scatter_rows(block_skip, device_count, GATHER_X_LAST)
        part_qkv = scatter_rows(block_qkv, device_count, GATHER_Y_LAST)
        part_out = scatter_rows(block_out, device_count, GATHER_X_LAST)
        part_up = scatter_rows(block_up, device_count, GATHER_Y_LAST)
        part_down = scatter_rows(block_down, device_count, GATHER_X_LAST)
        small_sums = sum_everywhere(small, device_count)
    grad_gains, grad_biases = small_sums[:2], small_sums[2:]
    return (
        layer_out,
        grad_in,
        grad_skip,
        part_skip,
        part_qkv,
        part_out,
        part_up,
        part_down,
        grad_gains,
        grad_biases,
    )


def solution(mesh):
    placed = (
        P(("dp", "sub"), None, None),
        P(("dp", "sub"), None, None),
        P(("dp", "sub")),
        P(("dp", "sub"), None, None),
        P(("dp", "sub")),
        P(("dp", "sub")),
        P(("dp", "sub")),
        P(("dp", "sub")),
        P(("dp", "sub")),
        P(),
        P(),
    )
    mesh_sizes = (mesh.shape["dp"], mesh.shape["sub"])
    return jax.shard_map(
        functools.partial(on_device, mesh_sizes),
        mesh=mesh,
        in_specs=placed,
        out_specs=(
            P(("dp", "sub"), None, None),
            P(("dp", "sub"), None, None),
            P(("dp", "sub"), None, None),
            P(("dp", "sub")),
            P(("dp", "sub")),
            P(("dp", "sub")),
            P(("dp", "sub")),
            P(("dp", "sub")),
            P(),
            P(),
        ),
        check_vma=False,
    )
```

```python
import functools

import jax
import jax.numpy as jnp
from jax import lax
from jax.experimental import pallas as pl
from jax.experimental.pallas import tpu as pltpu
from jax.sharding import PartitionSpec as P


HEADS = 16
HD = 72
FF = 4608


norm_epsilon = 1e-05
masked_score = -1e30


def product(left_side, right_side):
    return jnp.dot(left_side, right_side, preferred_element_type=jnp.float32)


def cross_rows(left_side, right_side):
    return lax.dot_general(
        left_side, right_side, (((0,), (0,)), ((), ())), preferred_element_type=jnp.float32
    )


def cross_cols(left_side, right_side):
    return lax.dot_general(
        left_side, right_side, (((1,), (1,)), ((), ())), preferred_element_type=jnp.float32
    )


FLAT_AXES = ("dp", "sub")
GATHER_X_LAST = (3, 4, 1, 2, 0)
GATHER_Y_LAST = (3, 4, 2, 1, 0)


def bit_order(device_count, wanted):
    bits = device_count.bit_length() - 1
    return wanted if bits == len(wanted) else tuple(range(bits))


def swap_with(array, bit, device_count):
    pairs = [(place, place ^ (1 << bit)) for place in range(device_count)]
    return lax.ppermute(array, FLAT_AXES, pairs)


def own_bit(bit):
    return (lax.axis_index(FLAT_AXES) >> bit) & 1


def can_halve(row_count, device_count):
    return device_count & (device_count - 1) == 0 and row_count % device_count == 0


def gather_rows(flat_shard, row_count, column_count, device_count, wanted):
    if not can_halve(row_count, device_count):
        whole = lax.all_gather(flat_shard, FLAT_AXES, axis=0, tiled=True)
        return whole.reshape(row_count, column_count)
    shard_rows = row_count // device_count
    held = flat_shard.reshape(1, shard_rows, column_count)
    done = []
    for bit in bit_order(device_count, wanted):
        other = swap_with(held, bit, device_count)
        low = sum(1 for place in done if place < bit)
        shape = (-1, 1, 2**low, shard_rows, column_count)
        first = own_bit(bit) == 0
        mine, theirs = held.reshape(shape), other.reshape(shape)
        held = jnp.concatenate(
            [jnp.where(first, mine, theirs), jnp.where(first, theirs, mine)], 1
        )
        held = held.reshape(-1, shard_rows, column_count)
        done.append(bit)
    return held.reshape(row_count, column_count)


def scatter_rows(block, device_count, wanted):
    row_count, column_count = block.shape
    if not can_halve(row_count, device_count):
        return lax.psum_scatter(
            block.reshape(-1), FLAT_AXES, scatter_dimension=0, tiled=True
        )
    shard_rows = row_count // device_count
    held = block.astype(jnp.bfloat16).reshape(device_count, shard_rows, column_count)
    left = set(range(device_count.bit_length() - 1))
    for bit in reversed(bit_order(device_count, wanted)):
        left.remove(bit)
        low = sum(1 for place in left if place < bit)
        shape = (-1, 2, 2**low * shard_rows, column_count)
        halves = held.reshape(shape)
        mine = own_bit(bit)
        sent = lax.dynamic_index_in_dim(halves, 1 - mine, 1, keepdims=False)
        kept = lax.dynamic_index_in_dim(halves, mine, 1, keepdims=False)
        got = swap_with(sent, bit, device_count)
        total = kept.astype(jnp.float32) + got.astype(jnp.float32)
        held = total.astype(jnp.bfloat16) if left else total
    return held.reshape(-1)


def sum_everywhere(block, device_count):
    if device_count & (device_count - 1):
        return lax.psum(block, FLAT_AXES)
    for bit in range(device_count.bit_length() - 1):
        block = block + swap_with(block, bit, device_count)
    return block


MESH_IDS = pl.DeviceIdType.MESH


def place_of():
    spread, near = lax.axis_index("dp"), lax.axis_index("sub")
    return spread // 2, spread % 2, near // 2, near % 2


def device_at(place):
    z, x, y, core = place
    return (z * 2 + x, y * 2 + core)


def partner_of(place, step):
    z, x, y, core = place
    if step == "z1":
        return (z + 1 - 2 * (z % 2), x, y, core)
    if step == "z2":
        return (z + 2 - 4 * (z // 2), x, y, core)
    if step == "x":
        return (z, 1 - x, y, core)
    if step == "y":
        return (z, x, 1 - y, core)
    return (z, x, y, 1 - core)


ALL_STEPS = ("z1", "z2", "x", "y", "core")


def greet_partners(place):
    barrier = pltpu.get_barrier_semaphore()
    for step in ALL_STEPS:
        pl.semaphore_signal(
            barrier,
            inc=1,
            device_id=device_at(partner_of(place, step)),
            device_id_type=MESH_IDS,
        )
    pl.semaphore_wait(barrier, len(ALL_STEPS))


def held_region(whole, place, step, last):
    z, x, y, core = place
    if step == "z1":
        return whole.at[z, x, y]
    if step == "z2":
        return whole.at[pl.ds(2 * (z // 2), 2), x, y]
    if step == "core":
        return whole
    if step != last:
        return whole.at[:, x, y]
    if step == "x":
        return whole.at[:, x]
    return whole.at[:, :, y]


SKIP, QKV, OUT, UP, DOWN = range(5)
PIECES = (
    (QKV, "columns", 2, 0, 25, 2, 0, 25, "y"),
    (OUT, "columns", 2, 3, 4, 1, 3, 5, "x"),
    (QKV, "columns", 2, 2, 23, 2, 2, 23, "y"),
    (OUT, "columns", 3, 0, 6, 3, 0, 6, "x"),
    (QKV, "columns", 5, 9, 13, 4, 9, 14, "y"),
    (SKIP, "rows", 24, 48, 48, 24, 48, 48, "x"),
    (QKV, "columns", 5, 4, 18, 5, 4, 18, "y"),
    (SKIP, "rows", 48, 0, 0, 48, 0, 0, "x"),
    (UP, "columns", 6, 0, 18, 6, 0, 18, "y"),
    (DOWN, "rows", 48, 0, 0, 48, 0, 0, "x"),
    (UP, "columns", 6, 6, 24, 6, 6, 24, "y"),
    (DOWN, "rows", 48, 48, 48, 48, 48, 48, "x"),
    (UP, "columns", 6, 12, 30, 6, 12, 30, "y"),
    (DOWN, "rows", 48, 96, 96, 48, 96, 96, "x"),
)
PIECE_GROUPS = (0, 0, 1, 1, 2, 2, 3, 3, 4, 4, 5, 5, 6, 6)
GROUP_COUNT = 7
PIECE_COUNT = len(PIECES)
WINDOW_FIRST = {QKV: (0, 13), OUT: (0, 4), UP: (0, 18)}


def piece_columns(size, first_zero, first_one, owner):
    first = 128 * (first_zero + owner * (first_one - first_zero))
    return pl.ds(pl.multiple_of(first, 128), 128 * size)


def piece_window(whole, piece, owner):
    _, axis, size, first_zero, first_one = piece[:5]
    if axis == "rows":
        return whole.at[:, :, :, owner, pl.ds(first_zero, size)]
    return whole.at[:, :, :, :, piece_columns(size, first_zero, first_one, owner)]


def gather_kernel(
    skip_in, qkv_in, out_in, up_in, down_in,
    skip_out, qkv_out, out_out, up_out, down_out,
    local_sems, send_sems, recv_sems,
):
    place = place_of()
    core = place[3]
    sources = (skip_in, qkv_in, out_in, up_in, down_in)
    targets = (skip_out, qkv_out, out_out, up_out, down_out)
    items = []
    for piece in PIECES:
        weight, axis, size, first_zero, first_one = piece[:5]
        window = piece_window(targets[weight], piece, core)
        if axis == "rows":
            source, passed = sources[weight].at[pl.ds(first_zero, size)], window
        else:
            source = sources[weight].at[:, piece_columns(size, first_zero, first_one, core)]
            passed = targets[weight].at[:, :, :, :, piece_columns(*piece[5:8], core)]
        items.append((source, window, passed, piece[8]))

    def local_copy(index):
        source, whole, _, _ = items[index]
        z, x, y, _ = place
        return pltpu.make_async_copy(source, whole.at[z, x, y], local_sems.at[index])

    def remote_copy(index, phase):
        source, whole, passed, last = items[index]
        steps = ("z1", "z2") + (("x", "y") if last == "y" else ("y", "x")) + ("core",)
        step = steps[phase]
        target = held_region(passed if step == "core" else whole, place, step, last)
        return pltpu.make_async_remote_copy(
            src_ref=source if phase == 0 else target,
            dst_ref=target,
            send_sem=send_sems.at[index, phase],
            recv_sem=recv_sems.at[index, phase],
            device_id=device_at(partner_of(place, step)),
            device_id_type=MESH_IDS,
        )

    for index in range(len(items)):
        local_copy(index).start()
    greet_partners(place)
    for slot in range(GROUP_COUNT + 4):
        for phase, index in (
            (phase, index)
            for phase in (0, 1, 3, 2, 4)
            for index in range(PIECE_COUNT)
            if PIECE_GROUPS[index] == slot - phase
        ):
            if phase == 1:
                local_copy(index).wait()
            if phase > 0:
                remote_copy(index, phase - 1).wait_recv()
            remote_copy(index, phase).start()
    for index in range(len(items)):
        remote_copy(index, 4).wait_recv()
    for index in range(len(items)):
        for phase in range(5):
            remote_copy(index, phase).wait_send()


def join_core_pair(shard, device_count):
    other = swap_with(shard, 0, device_count)
    first = own_bit(0) == 0
    return jnp.concatenate(
        [jnp.where(first, shard, other), jnp.where(first, other, shard)], 0
    )


def gather_weights(w_skip, w_qkv, w_out, w_up, w_down, model_width, hidden_width, device_count):
    sources = (
        w_skip.reshape(-1, model_width),
        join_core_pair(w_qkv.reshape(-1, 3 * model_width), device_count),
        join_core_pair(w_out.reshape(-1, model_width), device_count),
        join_core_pair(w_up.reshape(-1, hidden_width), device_count),
        w_down.reshape(-1, model_width),
    )
    leads = ((4, 2, 2, 2), (4, 2, 2), (4, 2, 2), (4, 2, 2), (4, 2, 2, 2))
    wholes = pl.pallas_call(
        gather_kernel,
        out_shape=[
            jax.ShapeDtypeStruct(lead + source.shape, source.dtype)
            for lead, source in zip(leads, sources)
        ],
        in_specs=[pl.BlockSpec(memory_space=pltpu.VMEM)] * 5,
        out_specs=[pl.BlockSpec(memory_space=pl.ANY)] * 5,
        scratch_shapes=[
            pltpu.SemaphoreType.DMA((PIECE_COUNT,)),
            pltpu.SemaphoreType.DMA((PIECE_COUNT, 5)),
            pltpu.SemaphoreType.DMA((PIECE_COUNT, 5)),
        ],
        compiler_params=pltpu.CompilerParams(collective_id=0, has_side_effects=True),
        name="gather_weights",
    )(*sources)
    return tuple(whole.reshape(-1, whole.shape[-1]) for whole in wholes)


def tuned_mesh(mesh_sizes, model_width, hidden_width):
    return mesh_sizes == (8, 4) and (model_width, hidden_width) == (1152, 4608)


SCATTER_GROUPS = tuple(GROUP_COUNT - 1 - group for group in PIECE_GROUPS)
SCATTER_SHAPES = tuple(
    (piece[2], 1152) if piece[1] == "rows" else (72, 128 * piece[2]) for piece in PIECES
)
RESULT_SHAPES = ((72, 1152), (72, 1792), (72, 640), (72, 2304), (144, 1152))
SMALL_ROWS = 16


def scatter_kernel(
    skip_grad, qkv_grad, out_grad, up_grad, down_grad, small_in, *rest
):
    item_count = len(SCATTER_SHAPES)
    results, rest = rest[:5], rest[5:]
    small_out, rest = rest[0], rest[1:]
    sums, rest = rest[:item_count], rest[item_count:]
    arrived, rest = rest[: 5 * item_count], rest[5 * item_count :]
    small_held, small_arrived, local_sems, send_sems, recv_sems, small_send, small_recv = rest
    place = place_of()
    z, x, y, core = place
    other_core = 1 - core

    grads = (skip_grad, qkv_grad, out_grad, up_grad, down_grad)

    def source(index, owner):
        return piece_window(grads[PIECES[index][0]], PIECES[index], owner)

    def result_window(index):
        weight, axis, size, first_zero, first_one = PIECES[index][:5]
        if axis == "rows":
            return results[weight].at[pl.ds(first_zero, size)]
        low, high = WINDOW_FIRST[weight]
        spot = piece_columns(size, first_zero - low, first_one - high, core)
        return results[weight].at[:, spot]

    def steps_of(index):
        middle = ("y", "x") if PIECES[index][8] == "y" else ("x", "y")
        return ("core",) + middle + ("z2", "z1")

    def sent_region(index, phase):
        held = sums[index]
        step = steps_of(index)[phase]
        if step == "core":
            return source(index, other_core)
        if step == "z2":
            return held.at[pl.ds(2 - 2 * (z // 2), 2), x, y]
        if step == "z1":
            return held.at[z + 1 - 2 * (z % 2), x, y]
        if step == "x":
            return held.at[:, 1 - x] if phase == 1 else held.at[:, 1 - x, y]
        return held.at[:, :, 1 - y] if phase == 1 else held.at[:, x, 1 - y]

    def local_copy(index):
        return pltpu.make_async_copy(
            source(index, core), sums[index], local_sems.at[index]
        )

    def remote_copy(index, phase):
        return pltpu.make_async_remote_copy(
            src_ref=sent_region(index, phase),
            dst_ref=arrived[5 * index + phase],
            send_sem=send_sems.at[index, phase],
            recv_sem=recv_sems.at[index, phase],
            device_id=device_at(partner_of(place, steps_of(index)[phase])),
            device_id_type=MESH_IDS,
        )

    def small_copy(phase):
        return pltpu.make_async_remote_copy(
            src_ref=small_held.at[phase],
            dst_ref=small_arrived.at[phase],
            send_sem=small_send.at[phase],
            recv_sem=small_recv.at[phase],
            device_id=device_at(partner_of(place, ALL_STEPS[phase])),
            device_id_type=MESH_IDS,
        )

    def add_arrived(index, phase):
        held, got = sums[index], arrived[5 * index + phase]
        step = steps_of(index)[phase]

        def total(mine, theirs):
            return mine.astype(jnp.float32) + theirs.astype(jnp.float32)

        if step == "z1":
            result_window(index)[...] = total(held[z, x, y], got[...])
            return

        def one(turn, carry):
            if step == "core":
                spot = (turn // 4, (turn // 2) % 2, turn % 2)
                taken = got[turn // 4, (turn // 2) % 2, turn % 2]
            elif step == "z2":
                spot, taken = (2 * (z // 2) + turn, x, y), got[turn]
            elif phase == 2:
                spot, taken = (turn, x, y), got[turn]
            elif step == "x":
                spot, taken = (turn // 2, x, turn % 2), got[turn // 2, turn % 2]
            else:
                spot, taken = (turn // 2, turn % 2, y), got[turn // 2, turn % 2]
            held[spot] = total(held[spot], taken).astype(jnp.bfloat16)
            return carry

        lax.fori_loop(0, (16, 8, 4, 2)[phase], one, 0)

    for index in reversed(range(item_count)):
        local_copy(index).start()
    small_held[0] = small_in[...]
    greet_partners(place)
    for index in reversed(range(item_count)):
        remote_copy(index, 0).start()
    small_copy(0).start()
    for slot in range(GROUP_COUNT + 4):
        for index in range(item_count):
            phase = slot - SCATTER_GROUPS[index]
            if phase < 0 or phase > 4:
                continue
            if phase == 0:
                local_copy(index).wait()
            remote_copy(index, phase).wait_recv()
            add_arrived(index, phase)
            if phase < 4:
                remote_copy(index, phase + 1).start()
        if slot < 5:
            small_copy(slot).wait_recv()
            summed = small_held[slot] + small_arrived[slot]
            if slot < 4:
                small_held[slot + 1] = summed
                small_copy(slot + 1).start()
            else:
                small_out[...] = summed
    for phase in range(5):
        small_copy(phase).wait_send()
        for index in range(item_count):
            remote_copy(index, phase).wait_send()


def split_core_pair(window, row_count, column_count, passed, device_count):
    core = own_bit(0)
    kept_rows = lax.dynamic_slice_in_dim(window, core * row_count, row_count, 0)
    sent_rows = lax.dynamic_slice_in_dim(window, (1 - core) * row_count, row_count, 0)
    got = swap_with(sent_rows, 0, device_count)
    first = core == 0
    left = jnp.concatenate([kept_rows, got[:, got.shape[1] - passed :]], 1)
    right = jnp.concatenate([got[:, :passed], kept_rows], 1)
    return jnp.where(first, left, right).reshape(-1)


def scatter_gradients(skip_grad, qkv_grad, out_grad, up_grad, down_grad, small, device_count):
    blocks = [
        block.astype(jnp.bfloat16).reshape(lead + (-1, block.shape[-1]))
        for block, lead in (
            (skip_grad, (4, 2, 2, 2)),
            (qkv_grad, (4, 2, 2)),
            (out_grad, (4, 2, 2)),
            (up_grad, (4, 2, 2)),
            (down_grad, (4, 2, 2, 2)),
        )
    ]
    small_count, width = small.shape
    padded = jnp.pad(small, ((0, SMALL_ROWS - small_count), (0, 0)))
    leads = ((4, 2, 2), (4, 2), (4,), (2,), ())
    item_count = len(SCATTER_SHAPES)
    outcome = pl.pallas_call(
        scatter_kernel,
        out_shape=[jax.ShapeDtypeStruct(shape, jnp.float32) for shape in RESULT_SHAPES]
        + [jax.ShapeDtypeStruct((SMALL_ROWS, width), jnp.float32)],
        in_specs=[pl.BlockSpec(memory_space=pl.ANY)] * 5
        + [pl.BlockSpec(memory_space=pltpu.VMEM)],
        out_specs=[pl.BlockSpec(memory_space=pltpu.VMEM)] * 6,
        scratch_shapes=[
            pltpu.VMEM((4, 2, 2) + shape, jnp.bfloat16) for shape in SCATTER_SHAPES
        ]
        + [
            pltpu.VMEM(lead + shape, jnp.bfloat16)
            for shape in SCATTER_SHAPES
            for lead in leads
        ]
        + [
            pltpu.VMEM((5, SMALL_ROWS, width), jnp.float32),
            pltpu.VMEM((5, SMALL_ROWS, width), jnp.float32),
            pltpu.SemaphoreType.DMA((item_count,)),
            pltpu.SemaphoreType.DMA((item_count, 5)),
            pltpu.SemaphoreType.DMA((item_count, 5)),
            pltpu.SemaphoreType.DMA((5,)),
            pltpu.SemaphoreType.DMA((5,)),
        ],
        compiler_params=pltpu.CompilerParams(
            collective_id=1, has_side_effects=True, vmem_limit_bytes=66_000_000
        ),
        name="scatter_gradients",
    )(*blocks, padded)
    skip_part, qkv_part, out_part, up_part, down_part, summed = outcome
    part_up = split_core_pair(up_part, 36, 4608, 2304, device_count)
    part_qkv = split_core_pair(qkv_part, 36, 3456, 1664, device_count)
    part_out = split_core_pair(out_part, 36, 1152, 512, device_count)
    part_down = down_part.reshape(-1)
    return (
        skip_part.reshape(-1), part_qkv, part_out, part_up, part_down, summed[:small_count]
    )


def norm_forward(stream, gain_row, shift_row):
    centred = stream - jnp.mean(stream, -1, keepdims=True)
    inverse = lax.rsqrt(jnp.mean(centred * centred, -1, keepdims=True) + norm_epsilon)
    normal = centred * inverse
    return (normal * gain_row + shift_row, normal, inverse)


def norm_backward(incoming, normal, inverse, gain_row):
    grad_gain = jnp.sum(incoming * normal, 0)
    grad_shift = jnp.sum(incoming, 0)
    scaled = incoming * gain_row
    centred = scaled - jnp.mean(scaled, -1, keepdims=True)
    grad_value = inverse * (centred - normal * jnp.mean(scaled * normal, -1, keepdims=True))
    return (grad_value, grad_gain, grad_shift)


def gelu_and_slope(hidden):
    cumulative = 0.5 * (1.0 + lax.erf(hidden * 0.5**0.5))
    density = jnp.exp(-0.5 * hidden * hidden) * (2.0 * jnp.pi) ** (-0.5)
    active = (hidden * cumulative).astype(jnp.bfloat16)
    return lax.optimization_barrier((active, cumulative + hidden * density))


def attention_shares(queries, key_rows, key_valid, score_scale):
    scores = (
        jnp.einsum("ishd,ithd->ihst", queries, key_rows, preferred_element_type=jnp.float32)
        * score_scale
    )
    scores = jnp.where(key_valid[:, None, None, :], scores, masked_score)
    highest = jnp.max(scores, -1, keepdims=True)
    raised = jnp.exp(scores - highest)
    return raised / jnp.sum(raised, -1, keepdims=True)


def on_device(
    mesh_sizes,
    block_in,
    long_skip,
    lengths,
    grad_out,
    w_skip,
    w_qkv,
    w_out,
    w_up,
    w_down,
    norm_gains,
    biases,
):
    item_count, slot_count, model_width = block_in.shape
    device_count = mesh_sizes[0] * mesh_sizes[1]
    row_count = item_count * slot_count
    head_count = HEADS
    head_size = HD
    hidden_width = FF
    score_scale = HD ** (-0.5)
    key_valid = jnp.arange(slot_count, dtype=jnp.int32)[None, :] < lengths[:, None] + 2
    if tuned_mesh(mesh_sizes, model_width, hidden_width):
        skip_full, qkv_full, out_full, up_full, down_full = gather_weights(
            w_skip, w_qkv, w_out, w_up, w_down, model_width, hidden_width, device_count
        )
    else:
        skip_full = gather_rows(
            w_skip, 2 * model_width, model_width, device_count, GATHER_X_LAST
        )
        qkv_full = gather_rows(
            w_qkv, model_width, 3 * model_width, device_count, GATHER_Y_LAST
        )
        out_full = gather_rows(w_out, model_width, model_width, device_count, GATHER_X_LAST)
        up_full = gather_rows(w_up, model_width, hidden_width, device_count, GATHER_Y_LAST)
        down_full = gather_rows(w_down, hidden_width, model_width, device_count, GATHER_X_LAST)
    joined = jnp.concatenate([block_in, long_skip], -1).reshape(row_count, 2 * model_width)
    stream_one = product(joined, skip_full) + biases[0]
    normed, normal_one, inverse_one = norm_forward(stream_one, norm_gains[0], biases[1])
    normed_low = normed.astype(jnp.bfloat16)
    triple = product(normed_low, qkv_full).astype(jnp.bfloat16)
    triple = triple.reshape(item_count, slot_count, 3, head_count, head_size)
    queries = triple[:, :, 0]
    key_rows = triple[:, :, 1]
    values = triple[:, :, 2]
    shares = attention_shares(queries, key_rows, key_valid, score_scale)
    shares_low = shares.astype(jnp.bfloat16)
    mixture = jnp.einsum("ihst,ithd->ishd", shares_low, values, preferred_element_type=jnp.float32)
    mixture_low = mixture.reshape(row_count, model_width).astype(jnp.bfloat16)
    stream_two = stream_one + (product(mixture_low, out_full) + biases[2])
    normed_two, normal_two, inverse_two = norm_forward(stream_two, norm_gains[1], biases[3])
    normed_two_low = normed_two.astype(jnp.bfloat16)
    hidden = product(normed_two_low, up_full) + biases[4:8].reshape(hidden_width)
    active_low, slope = gelu_and_slope(hidden)
    result = stream_two + (product(active_low, down_full) + biases[8])
    layer_out = result.astype(jnp.bfloat16).reshape(item_count, slot_count, model_width)
    row_mask = key_valid.reshape(row_count, 1).astype(jnp.float32)
    start_grad = grad_out.reshape(row_count, model_width).astype(jnp.float32) * row_mask
    grad_branch = start_grad.astype(jnp.bfloat16)
    bias_down = jnp.sum(grad_branch.astype(jnp.float32), 0)
    block_down = cross_rows(active_low, grad_branch)
    grad_active = cross_cols(grad_branch, down_full)
    grad_hidden = (grad_active * slope).astype(jnp.bfloat16)
    bias_up = jnp.sum(grad_hidden.astype(jnp.float32), 0)
    block_up = cross_rows(normed_two_low, grad_hidden)
    grad_normed_two = cross_cols(grad_hidden, up_full)
    local_two, gain_two, shift_two = norm_backward(
        grad_normed_two, normal_two, inverse_two, norm_gains[1]
    )
    grad_two = start_grad + local_two
    grad_attn = grad_two.astype(jnp.bfloat16)
    bias_out = jnp.sum(grad_attn.astype(jnp.float32), 0)
    block_out = cross_rows(mixture_low, grad_attn)
    grad_mixture = cross_cols(grad_attn, out_full).astype(jnp.bfloat16)
    grad_mixture = grad_mixture.reshape(item_count, slot_count, head_count, head_size)
    grad_shares = jnp.einsum(
        "ishd,ithd->ihst", grad_mixture, values, preferred_element_type=jnp.float32
    )
    grad_scores = shares * (grad_shares - jnp.sum(shares * grad_shares, -1, keepdims=True))
    grad_scores_low = grad_scores.astype(jnp.bfloat16)
    grad_queries = (
        jnp.einsum("ihst,ithd->ishd", grad_scores_low, key_rows, preferred_element_type=jnp.float32)
        * score_scale
    )
    grad_keys = (
        jnp.einsum("ihst,ishd->ithd", grad_scores_low, queries, preferred_element_type=jnp.float32)
        * score_scale
    )
    grad_values = jnp.einsum(
        "ihst,ishd->ithd", shares_low, grad_mixture, preferred_element_type=jnp.float32
    )
    grad_triple = jnp.stack([grad_queries, grad_keys, grad_values], 2).astype(jnp.bfloat16)
    grad_triple = grad_triple.reshape(row_count, 3 * model_width)
    block_qkv = cross_rows(normed_low, grad_triple)
    grad_normed = cross_cols(grad_triple, qkv_full)
    local_one, gain_one, shift_one = norm_backward(
        grad_normed, normal_one, inverse_one, norm_gains[0]
    )
    grad_one = (grad_two + local_one).astype(jnp.bfloat16)
    bias_skip = jnp.sum(grad_one.astype(jnp.float32), 0)
    block_skip = cross_rows(joined, grad_one)
    grad_joined = cross_cols(grad_one, skip_full).reshape(item_count, slot_count, 2 * model_width)
    grad_in = grad_joined[:, :, :model_width].astype(jnp.bfloat16)
    grad_skip = grad_joined[:, :, model_width:].astype(jnp.bfloat16)
    gains_part = jnp.stack([gain_one, gain_two], 0)
    biases_part = jnp.concatenate(
        [
            jnp.stack([bias_skip, shift_one, bias_out, shift_two], 0),
            bias_up.reshape(4, model_width),
            bias_down[None, :],
        ],
        0,
    )
    small = jnp.concatenate([gains_part, biases_part], 0)
    if tuned_mesh(mesh_sizes, model_width, hidden_width):
        part_skip, part_qkv, part_out, part_up, part_down, small_sums = scatter_gradients(
            block_skip, block_qkv, block_out, block_up, block_down, small, device_count
        )
    else:
        part_skip = scatter_rows(block_skip, device_count, GATHER_X_LAST)
        part_qkv = scatter_rows(block_qkv, device_count, GATHER_Y_LAST)
        part_out = scatter_rows(block_out, device_count, GATHER_X_LAST)
        part_up = scatter_rows(block_up, device_count, GATHER_Y_LAST)
        part_down = scatter_rows(block_down, device_count, GATHER_X_LAST)
        small_sums = sum_everywhere(small, device_count)
    grad_gains, grad_biases = small_sums[:2], small_sums[2:]
    return (
        layer_out,
        grad_in,
        grad_skip,
        part_skip,
        part_qkv,
        part_out,
        part_up,
        part_down,
        grad_gains,
        grad_biases,
    )


def solution(mesh):
    placed = (
        P(("dp", "sub"), None, None),
        P(("dp", "sub"), None, None),
        P(("dp", "sub")),
        P(("dp", "sub"), None, None),
        P(("dp", "sub")),
        P(("dp", "sub")),
        P(("dp", "sub")),
        P(("dp", "sub")),
        P(("dp", "sub")),
        P(),
        P(),
    )
    mesh_sizes = (mesh.shape["dp"], mesh.shape["sub"])
    return jax.shard_map(
        functools.partial(on_device, mesh_sizes),
        mesh=mesh,
        in_specs=placed,
        out_specs=(
            P(("dp", "sub"), None, None),
            P(("dp", "sub"), None, None),
            P(("dp", "sub"), None, None),
            P(("dp", "sub")),
            P(("dp", "sub")),
            P(("dp", "sub")),
            P(("dp", "sub")),
            P(("dp", "sub")),
            P(),
            P(),
        ),
        check_vma=False,
    )
```

```python
import functools

import jax
import jax.numpy as jnp
from jax import lax
from jax.experimental import pallas as pl
from jax.experimental.pallas import tpu as pltpu
from jax.sharding import PartitionSpec as P


HEADS = 16
HD = 72
FF = 4608


norm_epsilon = 1e-05
masked_score = -1e30


def product(left_side, right_side):
    return jnp.dot(left_side, right_side, preferred_element_type=jnp.float32)


def cross_rows(left_side, right_side):
    return lax.dot_general(
        left_side, right_side, (((0,), (0,)), ((), ())), preferred_element_type=jnp.float32
    )


def cross_cols(left_side, right_side):
    return lax.dot_general(
        left_side, right_side, (((1,), (1,)), ((), ())), preferred_element_type=jnp.float32
    )


FLAT_AXES = ("dp", "sub")
GATHER_X_LAST = (3, 4, 1, 2, 0)
GATHER_Y_LAST = (3, 4, 2, 1, 0)


def bit_order(device_count, wanted):
    bits = device_count.bit_length() - 1
    return wanted if bits == len(wanted) else tuple(range(bits))


def swap_with(array, bit, device_count):
    pairs = [(place, place ^ (1 << bit)) for place in range(device_count)]
    return lax.ppermute(array, FLAT_AXES, pairs)


def own_bit(bit):
    return (lax.axis_index(FLAT_AXES) >> bit) & 1


def can_halve(row_count, device_count):
    return device_count & (device_count - 1) == 0 and row_count % device_count == 0


def gather_rows(flat_shard, row_count, column_count, device_count, wanted):
    if not can_halve(row_count, device_count):
        whole = lax.all_gather(flat_shard, FLAT_AXES, axis=0, tiled=True)
        return whole.reshape(row_count, column_count)
    shard_rows = row_count // device_count
    held = flat_shard.reshape(1, shard_rows, column_count)
    done = []
    for bit in bit_order(device_count, wanted):
        other = swap_with(held, bit, device_count)
        low = sum(1 for place in done if place < bit)
        shape = (-1, 1, 2**low, shard_rows, column_count)
        first = own_bit(bit) == 0
        mine, theirs = held.reshape(shape), other.reshape(shape)
        held = jnp.concatenate(
            [jnp.where(first, mine, theirs), jnp.where(first, theirs, mine)], 1
        )
        held = held.reshape(-1, shard_rows, column_count)
        done.append(bit)
    return held.reshape(row_count, column_count)


def scatter_rows(block, device_count, wanted):
    row_count, column_count = block.shape
    if not can_halve(row_count, device_count):
        return lax.psum_scatter(
            block.reshape(-1), FLAT_AXES, scatter_dimension=0, tiled=True
        )
    shard_rows = row_count // device_count
    held = block.astype(jnp.bfloat16).reshape(device_count, shard_rows, column_count)
    left = set(range(device_count.bit_length() - 1))
    for bit in reversed(bit_order(device_count, wanted)):
        left.remove(bit)
        low = sum(1 for place in left if place < bit)
        shape = (-1, 2, 2**low * shard_rows, column_count)
        halves = held.reshape(shape)
        mine = own_bit(bit)
        sent = lax.dynamic_index_in_dim(halves, 1 - mine, 1, keepdims=False)
        kept = lax.dynamic_index_in_dim(halves, mine, 1, keepdims=False)
        got = swap_with(sent, bit, device_count)
        total = kept.astype(jnp.float32) + got.astype(jnp.float32)
        held = total.astype(jnp.bfloat16) if left else total
    return held.reshape(-1)


def sum_everywhere(block, device_count):
    if device_count & (device_count - 1):
        return lax.psum(block, FLAT_AXES)
    for bit in range(device_count.bit_length() - 1):
        block = block + swap_with(block, bit, device_count)
    return block


MESH_IDS = pl.DeviceIdType.MESH


def place_of():
    spread, near = lax.axis_index("dp"), lax.axis_index("sub")
    return spread // 2, spread % 2, near // 2, near % 2


def device_at(place):
    z, x, y, core = place
    return (z * 2 + x, y * 2 + core)


def partner_of(place, step):
    z, x, y, core = place
    if step == "z1":
        return (z + 1 - 2 * (z % 2), x, y, core)
    if step == "z2":
        return (z + 2 - 4 * (z // 2), x, y, core)
    if step == "x":
        return (z, 1 - x, y, core)
    if step == "y":
        return (z, x, 1 - y, core)
    return (z, x, y, 1 - core)


ALL_STEPS = ("z1", "z2", "x", "y", "core")


def greet_partners(place):
    barrier = pltpu.get_barrier_semaphore()
    for step in ALL_STEPS:
        pl.semaphore_signal(
            barrier,
            inc=1,
            device_id=device_at(partner_of(place, step)),
            device_id_type=MESH_IDS,
        )
    pl.semaphore_wait(barrier, len(ALL_STEPS))


def held_region(whole, place, step, last):
    z, x, y, core = place
    if step == "z1":
        return whole.at[z, x, y]
    if step == "z2":
        return whole.at[pl.ds(2 * (z // 2), 2), x, y]
    if step == "core":
        return whole
    if step != last:
        return whole.at[:, x, y]
    if step == "x":
        return whole.at[:, x]
    return whole.at[:, :, y]


SKIP, QKV, OUT, UP, DOWN = range(5)
PIECES = (
    (QKV, "columns", 2, 0, 25, 2, 0, 25, "y"),
    (OUT, "columns", 2, 3, 4, 1, 3, 5, "x"),
    (QKV, "columns", 2, 2, 23, 2, 2, 23, "y"),
    (OUT, "columns", 3, 0, 6, 3, 0, 6, "x"),
    (QKV, "columns", 5, 9, 13, 4, 9, 14, "y"),
    (SKIP, "rows", 24, 48, 48, 24, 48, 48, "x"),
    (QKV, "columns", 5, 4, 18, 5, 4, 18, "y"),
    (SKIP, "rows", 48, 0, 0, 48, 0, 0, "x"),
    (UP, "columns", 6, 0, 18, 6, 0, 18, "y"),
    (DOWN, "rows", 48, 0, 0, 48, 0, 0, "x"),
    (UP, "columns", 6, 6, 24, 6, 6, 24, "y"),
    (DOWN, "rows", 48, 48, 48, 48, 48, 48, "x"),
    (UP, "columns", 6, 12, 30, 6, 12, 30, "y"),
    (DOWN, "rows", 48, 96, 96, 48, 96, 96, "x"),
)
PIECE_GROUPS = (0, 0, 1, 1, 2, 2, 3, 3, 4, 4, 5, 5, 6, 6)
GROUP_COUNT = 7
PIECE_COUNT = len(PIECES)
WINDOW_FIRST = {QKV: (0, 13), OUT: (0, 4), UP: (0, 18)}


def piece_columns(size, first_zero, first_one, owner):
    first = 128 * (first_zero + owner * (first_one - first_zero))
    return pl.ds(pl.multiple_of(first, 128), 128 * size)


def piece_window(whole, piece, owner):
    _, axis, size, first_zero, first_one = piece[:5]
    if axis == "rows":
        return whole.at[:, :, :, owner, pl.ds(first_zero, size)]
    return whole.at[:, :, :, :, piece_columns(size, first_zero, first_one, owner)]


def gather_kernel(
    skip_in, qkv_in, out_in, up_in, down_in,
    skip_out, qkv_out, out_out, up_out, down_out,
    local_sems, send_sems, recv_sems,
):
    place = place_of()
    core = place[3]
    sources = (skip_in, qkv_in, out_in, up_in, down_in)
    targets = (skip_out, qkv_out, out_out, up_out, down_out)
    items = []
    for piece in PIECES:
        weight, axis, size, first_zero, first_one = piece[:5]
        window = piece_window(targets[weight], piece, core)
        if axis == "rows":
            source, passed = sources[weight].at[pl.ds(first_zero, size)], window
        else:
            source = sources[weight].at[:, piece_columns(size, first_zero, first_one, core)]
            passed = targets[weight].at[:, :, :, :, piece_columns(*piece[5:8], core)]
        items.append((source, window, passed, piece[8]))

    def local_copy(index):
        source, whole, _, _ = items[index]
        z, x, y, _ = place
        return pltpu.make_async_copy(source, whole.at[z, x, y], local_sems.at[index])

    def remote_copy(index, phase):
        source, whole, passed, last = items[index]
        steps = ("z1", "z2") + (("x", "y") if last == "y" else ("y", "x")) + ("core",)
        step = steps[phase]
        target = held_region(passed if step == "core" else whole, place, step, last)
        return pltpu.make_async_remote_copy(
            src_ref=source if phase == 0 else target,
            dst_ref=target,
            send_sem=send_sems.at[index, phase],
            recv_sem=recv_sems.at[index, phase],
            device_id=device_at(partner_of(place, step)),
            device_id_type=MESH_IDS,
        )

    for index in range(len(items)):
        local_copy(index).start()
    greet_partners(place)
    for slot in range(GROUP_COUNT + 4):
        for phase, index in (
            (phase, index)
            for phase in (0, 1, 3, 2, 4)
            for index in range(PIECE_COUNT)
            if PIECE_GROUPS[index] == slot - phase
        ):
            if phase == 1:
                local_copy(index).wait()
            if phase > 0:
                remote_copy(index, phase - 1).wait_recv()
            remote_copy(index, phase).start()
    for index in range(len(items)):
        remote_copy(index, 4).wait_recv()
    for index in range(len(items)):
        for phase in range(5):
            remote_copy(index, phase).wait_send()


def join_core_pair(shard, device_count):
    other = swap_with(shard, 0, device_count)
    first = own_bit(0) == 0
    return jnp.concatenate(
        [jnp.where(first, shard, other), jnp.where(first, other, shard)], 0
    )


def gather_weights(w_skip, w_qkv, w_out, w_up, w_down, model_width, hidden_width, device_count):
    sources = (
        w_skip.reshape(-1, model_width),
        join_core_pair(w_qkv.reshape(-1, 3 * model_width), device_count),
        join_core_pair(w_out.reshape(-1, model_width), device_count),
        join_core_pair(w_up.reshape(-1, hidden_width), device_count),
        w_down.reshape(-1, model_width),
    )
    leads = ((4, 2, 2, 2), (4, 2, 2), (4, 2, 2), (4, 2, 2), (4, 2, 2, 2))
    wholes = pl.pallas_call(
        gather_kernel,
        out_shape=[
            jax.ShapeDtypeStruct(lead + source.shape, source.dtype)
            for lead, source in zip(leads, sources)
        ],
        in_specs=[pl.BlockSpec(memory_space=pltpu.VMEM)] * 5,
        out_specs=[pl.BlockSpec(memory_space=pl.ANY)] * 5,
        scratch_shapes=[
            pltpu.SemaphoreType.DMA((PIECE_COUNT,)),
            pltpu.SemaphoreType.DMA((PIECE_COUNT, 5)),
            pltpu.SemaphoreType.DMA((PIECE_COUNT, 5)),
        ],
        compiler_params=pltpu.CompilerParams(collective_id=0, has_side_effects=True),
        name="gather_weights",
    )(*sources)
    return tuple(whole.reshape(-1, whole.shape[-1]) for whole in wholes)


def tuned_mesh(mesh_sizes, model_width, hidden_width):
    return mesh_sizes == (8, 4) and (model_width, hidden_width) == (1152, 4608)


SCATTER_GROUPS = tuple(GROUP_COUNT - 1 - group for group in PIECE_GROUPS)
SCATTER_SHAPES = tuple(
    (piece[2], 1152) if piece[1] == "rows" else (72, 128 * piece[2]) for piece in PIECES
)
RESULT_SHAPES = ((72, 1152), (72, 1792), (72, 640), (72, 2304), (144, 1152))
SMALL_ROWS = 16


def scatter_kernel(
    skip_grad, qkv_grad, out_grad, up_grad, down_grad, small_in, *rest
):
    item_count = len(SCATTER_SHAPES)
    results, rest = rest[:5], rest[5:]
    small_out, rest = rest[0], rest[1:]
    sums, rest = rest[:item_count], rest[item_count:]
    arrived, rest = rest[: 5 * item_count], rest[5 * item_count :]
    small_held, small_arrived, local_sems, send_sems, recv_sems, small_send, small_recv = rest
    place = place_of()
    z, x, y, core = place
    other_core = 1 - core

    grads = (skip_grad, qkv_grad, out_grad, up_grad, down_grad)

    def source(index, owner):
        return piece_window(grads[PIECES[index][0]], PIECES[index], owner)

    def result_window(index):
        weight, axis, size, first_zero, first_one = PIECES[index][:5]
        if axis == "rows":
            return results[weight].at[pl.ds(first_zero, size)]
        low, high = WINDOW_FIRST[weight]
        spot = piece_columns(size, first_zero - low, first_one - high, core)
        return results[weight].at[:, spot]

    def steps_of(index):
        middle = ("y", "x") if PIECES[index][8] == "y" else ("x", "y")
        return ("core",) + middle + ("z2", "z1")

    def sent_region(index, phase):
        held = sums[index]
        step = steps_of(index)[phase]
        if step == "core":
            return source(index, other_core)
        if step == "z2":
            return held.at[pl.ds(2 - 2 * (z // 2), 2), x, y]
        if step == "z1":
            return held.at[z + 1 - 2 * (z % 2), x, y]
        if step == "x":
            return held.at[:, 1 - x] if phase == 1 else held.at[:, 1 - x, y]
        return held.at[:, :, 1 - y] if phase == 1 else held.at[:, x, 1 - y]

    def local_copy(index):
        return pltpu.make_async_copy(
            source(index, core), sums[index], local_sems.at[index]
        )

    def remote_copy(index, phase):
        return pltpu.make_async_remote_copy(
            src_ref=sent_region(index, phase),
            dst_ref=arrived[5 * index + phase],
            send_sem=send_sems.at[index, phase],
            recv_sem=recv_sems.at[index, phase],
            device_id=device_at(partner_of(place, steps_of(index)[phase])),
            device_id_type=MESH_IDS,
        )

    def small_copy(phase):
        return pltpu.make_async_remote_copy(
            src_ref=small_held.at[phase],
            dst_ref=small_arrived.at[phase],
            send_sem=small_send.at[phase],
            recv_sem=small_recv.at[phase],
            device_id=device_at(partner_of(place, ALL_STEPS[phase])),
            device_id_type=MESH_IDS,
        )

    def add_arrived(index, phase):
        held, got = sums[index], arrived[5 * index + phase]
        step = steps_of(index)[phase]

        def total(mine, theirs):
            return mine.astype(jnp.float32) + theirs.astype(jnp.float32)

        if step == "z1":
            result_window(index)[...] = total(held[z, x, y], got[...])
            return

        def one(turn, carry):
            if step == "core":
                spot = (turn // 4, (turn // 2) % 2, turn % 2)
                taken = got[turn // 4, (turn // 2) % 2, turn % 2]
            elif step == "z2":
                spot, taken = (2 * (z // 2) + turn, x, y), got[turn]
            elif phase == 2:
                spot, taken = (turn, x, y), got[turn]
            elif step == "x":
                spot, taken = (turn // 2, x, turn % 2), got[turn // 2, turn % 2]
            else:
                spot, taken = (turn // 2, turn % 2, y), got[turn // 2, turn % 2]
            held[spot] = total(held[spot], taken).astype(jnp.bfloat16)
            return carry

        lax.fori_loop(0, (16, 8, 4, 2)[phase], one, 0)

    for index in reversed(range(item_count)):
        local_copy(index).start()
    small_held[0] = small_in[...]
    greet_partners(place)
    for index in reversed(range(item_count)):
        remote_copy(index, 0).start()
    small_copy(0).start()
    for slot in range(GROUP_COUNT + 4):
        for index in range(item_count):
            phase = slot - SCATTER_GROUPS[index]
            if phase < 0 or phase > 4:
                continue
            if phase == 0:
                local_copy(index).wait()
            remote_copy(index, phase).wait_recv()
            add_arrived(index, phase)
            if phase < 4:
                remote_copy(index, phase + 1).start()
        if slot < 5:
            small_copy(slot).wait_recv()
            summed = small_held[slot] + small_arrived[slot]
            if slot < 4:
                small_held[slot + 1] = summed
                small_copy(slot + 1).start()
            else:
                small_out[...] = summed
    for phase in range(5):
        small_copy(phase).wait_send()
        for index in range(item_count):
            remote_copy(index, phase).wait_send()


def split_core_pair(window, row_count, column_count, passed, device_count):
    core = own_bit(0)
    kept_rows = lax.dynamic_slice_in_dim(window, core * row_count, row_count, 0)
    sent_rows = lax.dynamic_slice_in_dim(window, (1 - core) * row_count, row_count, 0)
    got = swap_with(sent_rows, 0, device_count)
    first = core == 0
    left = jnp.concatenate([kept_rows, got[:, got.shape[1] - passed :]], 1)
    right = jnp.concatenate([got[:, :passed], kept_rows], 1)
    return jnp.where(first, left, right).reshape(-1)


def scatter_gradients(skip_grad, qkv_grad, out_grad, up_grad, down_grad, small, device_count):
    blocks = [
        block.astype(jnp.bfloat16).reshape(lead + (-1, block.shape[-1]))
        for block, lead in (
            (skip_grad, (4, 2, 2, 2)),
            (qkv_grad, (4, 2, 2)),
            (out_grad, (4, 2, 2)),
            (up_grad, (4, 2, 2)),
            (down_grad, (4, 2, 2, 2)),
        )
    ]
    small_count, width = small.shape
    padded = jnp.pad(small, ((0, SMALL_ROWS - small_count), (0, 0)))
    leads = ((4, 2, 2), (4, 2), (4,), (2,), ())
    item_count = len(SCATTER_SHAPES)
    outcome = pl.pallas_call(
        scatter_kernel,
        out_shape=[jax.ShapeDtypeStruct(shape, jnp.float32) for shape in RESULT_SHAPES]
        + [jax.ShapeDtypeStruct((SMALL_ROWS, width), jnp.float32)],
        in_specs=[pl.BlockSpec(memory_space=pl.ANY)] * 5
        + [pl.BlockSpec(memory_space=pltpu.VMEM)],
        out_specs=[pl.BlockSpec(memory_space=pltpu.VMEM)] * 6,
        scratch_shapes=[
            pltpu.VMEM((4, 2, 2) + shape, jnp.bfloat16) for shape in SCATTER_SHAPES
        ]
        + [
            pltpu.VMEM(lead + shape, jnp.bfloat16)
            for shape in SCATTER_SHAPES
            for lead in leads
        ]
        + [
            pltpu.VMEM((5, SMALL_ROWS, width), jnp.float32),
            pltpu.VMEM((5, SMALL_ROWS, width), jnp.float32),
            pltpu.SemaphoreType.DMA((item_count,)),
            pltpu.SemaphoreType.DMA((item_count, 5)),
            pltpu.SemaphoreType.DMA((item_count, 5)),
            pltpu.SemaphoreType.DMA((5,)),
            pltpu.SemaphoreType.DMA((5,)),
        ],
        compiler_params=pltpu.CompilerParams(
            collective_id=1, has_side_effects=True, vmem_limit_bytes=66_000_000
        ),
        name="scatter_gradients",
    )(*blocks, padded)
    skip_part, qkv_part, out_part, up_part, down_part, summed = outcome
    part_up = split_core_pair(up_part, 36, 4608, 2304, device_count)
    part_qkv = split_core_pair(qkv_part, 36, 3456, 1664, device_count)
    part_out = split_core_pair(out_part, 36, 1152, 512, device_count)
    part_down = down_part.reshape(-1)
    return (
        skip_part.reshape(-1), part_qkv, part_out, part_up, part_down, summed[:small_count]
    )


def norm_forward(stream, gain_row, shift_row):
    centred = stream - jnp.mean(stream, -1, keepdims=True)
    inverse = lax.rsqrt(jnp.mean(centred * centred, -1, keepdims=True) + norm_epsilon)
    normal = centred * inverse
    return (normal * gain_row + shift_row, normal, inverse)


def norm_backward(incoming, normal, inverse, gain_row):
    grad_gain = jnp.sum(incoming * normal, 0)
    grad_shift = jnp.sum(incoming, 0)
    scaled = incoming * gain_row
    centred = scaled - jnp.mean(scaled, -1, keepdims=True)
    grad_value = inverse * (centred - normal * jnp.mean(scaled * normal, -1, keepdims=True))
    return (grad_value, grad_gain, grad_shift)


def gelu(hidden):
    return hidden * (0.5 * (1.0 + lax.erf(hidden * 0.5**0.5)))


def gelu_slope(hidden):
    cumulative = 0.5 * (1.0 + lax.erf(hidden * 0.5**0.5))
    density = jnp.exp(-0.5 * hidden * hidden) * (2.0 * jnp.pi) ** (-0.5)
    return cumulative + hidden * density


def attention_shares(queries, key_rows, key_valid, score_scale):
    scores = (
        jnp.einsum("ishd,ithd->ihst", queries, key_rows, preferred_element_type=jnp.float32)
        * score_scale
    )
    scores = jnp.where(key_valid[:, None, None, :], scores, masked_score)
    highest = jnp.max(scores, -1, keepdims=True)
    raised = jnp.exp(scores - highest)
    return raised / jnp.sum(raised, -1, keepdims=True)


def on_device(
    mesh_sizes,
    block_in,
    long_skip,
    lengths,
    grad_out,
    w_skip,
    w_qkv,
    w_out,
    w_up,
    w_down,
    norm_gains,
    biases,
):
    item_count, slot_count, model_width = block_in.shape
    device_count = mesh_sizes[0] * mesh_sizes[1]
    row_count = item_count * slot_count
    head_count = HEADS
    head_size = HD
    hidden_width = FF
    score_scale = HD ** (-0.5)
    key_valid = jnp.arange(slot_count, dtype=jnp.int32)[None, :] < lengths[:, None] + 2
    if tuned_mesh(mesh_sizes, model_width, hidden_width):
        skip_full, qkv_full, out_full, up_full, down_full = gather_weights(
            w_skip, w_qkv, w_out, w_up, w_down, model_width, hidden_width, device_count
        )
    else:
        skip_full = gather_rows(
            w_skip, 2 * model_width, model_width, device_count, GATHER_X_LAST
        )
        qkv_full = gather_rows(
            w_qkv, model_width, 3 * model_width, device_count, GATHER_Y_LAST
        )
        out_full = gather_rows(w_out, model_width, model_width, device_count, GATHER_X_LAST)
        up_full = gather_rows(w_up, model_width, hidden_width, device_count, GATHER_Y_LAST)
        down_full = gather_rows(w_down, hidden_width, model_width, device_count, GATHER_X_LAST)
    joined = jnp.concatenate([block_in, long_skip], -1).reshape(row_count, 2 * model_width)
    stream_one = product(joined, skip_full) + biases[0]
    normed, normal_one, inverse_one = norm_forward(stream_one, norm_gains[0], biases[1])
    normed_low = normed.astype(jnp.bfloat16)
    triple = product(normed_low, qkv_full).astype(jnp.bfloat16)
    triple = triple.reshape(item_count, slot_count, 3, head_count, head_size)
    queries = triple[:, :, 0]
    key_rows = triple[:, :, 1]
    values = triple[:, :, 2]
    shares = attention_shares(queries, key_rows, key_valid, score_scale)
    shares_low = shares.astype(jnp.bfloat16)
    mixture = jnp.einsum("ihst,ithd->ishd", shares_low, values, preferred_element_type=jnp.float32)
    mixture_low = mixture.reshape(row_count, model_width).astype(jnp.bfloat16)
    stream_two = stream_one + (product(mixture_low, out_full) + biases[2])
    normed_two, normal_two, inverse_two = norm_forward(stream_two, norm_gains[1], biases[3])
    normed_two_low = normed_two.astype(jnp.bfloat16)
    hidden = product(normed_two_low, up_full) + biases[4:8].reshape(hidden_width)
    active_low, hidden = lax.optimization_barrier(
        (gelu(hidden).astype(jnp.bfloat16), hidden)
    )
    result = stream_two + (product(active_low, down_full) + biases[8])
    layer_out = result.astype(jnp.bfloat16).reshape(item_count, slot_count, model_width)
    row_mask = key_valid.reshape(row_count, 1).astype(jnp.float32)
    start_grad = grad_out.reshape(row_count, model_width).astype(jnp.float32) * row_mask
    grad_branch = start_grad.astype(jnp.bfloat16)
    bias_down = jnp.sum(grad_branch.astype(jnp.float32), 0)
    block_down = cross_rows(active_low, grad_branch)
    grad_active = cross_cols(grad_branch, down_full)
    grad_hidden = (grad_active * gelu_slope(hidden)).astype(jnp.bfloat16)
    bias_up = jnp.sum(grad_hidden.astype(jnp.float32), 0)
    block_up = cross_rows(normed_two_low, grad_hidden)
    grad_normed_two = cross_cols(grad_hidden, up_full)
    local_two, gain_two, shift_two = norm_backward(
        grad_normed_two, normal_two, inverse_two, norm_gains[1]
    )
    grad_two = start_grad + local_two
    grad_attn = grad_two.astype(jnp.bfloat16)
    bias_out = jnp.sum(grad_attn.astype(jnp.float32), 0)
    block_out = cross_rows(mixture_low, grad_attn)
    grad_mixture = cross_cols(grad_attn, out_full).astype(jnp.bfloat16)
    grad_mixture = grad_mixture.reshape(item_count, slot_count, head_count, head_size)
    grad_shares = jnp.einsum(
        "ishd,ithd->ihst", grad_mixture, values, preferred_element_type=jnp.float32
    )
    grad_scores = shares * (grad_shares - jnp.sum(shares * grad_shares, -1, keepdims=True))
    grad_scores_low = grad_scores.astype(jnp.bfloat16)
    grad_queries = (
        jnp.einsum("ihst,ithd->ishd", grad_scores_low, key_rows, preferred_element_type=jnp.float32)
        * score_scale
    )
    grad_keys = (
        jnp.einsum("ihst,ishd->ithd", grad_scores_low, queries, preferred_element_type=jnp.float32)
        * score_scale
    )
    grad_values = jnp.einsum(
        "ihst,ishd->ithd", shares_low, grad_mixture, preferred_element_type=jnp.float32
    )
    grad_triple = jnp.stack([grad_queries, grad_keys, grad_values], 2).astype(jnp.bfloat16)
    grad_triple = grad_triple.reshape(row_count, 3 * model_width)
    block_qkv = cross_rows(normed_low, grad_triple)
    grad_normed = cross_cols(grad_triple, qkv_full)
    local_one, gain_one, shift_one = norm_backward(
        grad_normed, normal_one, inverse_one, norm_gains[0]
    )
    grad_one = (grad_two + local_one).astype(jnp.bfloat16)
    bias_skip = jnp.sum(grad_one.astype(jnp.float32), 0)
    block_skip = cross_rows(joined, grad_one)
    grad_joined = cross_cols(grad_one, skip_full).reshape(item_count, slot_count, 2 * model_width)
    grad_in = grad_joined[:, :, :model_width].astype(jnp.bfloat16)
    grad_skip = grad_joined[:, :, model_width:].astype(jnp.bfloat16)
    gains_part = jnp.stack([gain_one, gain_two], 0)
    biases_part = jnp.concatenate(
        [
            jnp.stack([bias_skip, shift_one, bias_out, shift_two], 0),
            bias_up.reshape(4, model_width),
            bias_down[None, :],
        ],
        0,
    )
    small = jnp.concatenate([gains_part, biases_part], 0)
    if tuned_mesh(mesh_sizes, model_width, hidden_width):
        part_skip, part_qkv, part_out, part_up, part_down, small_sums = scatter_gradients(
            block_skip, block_qkv, block_out, block_up, block_down, small, device_count
        )
    else:
        part_skip = scatter_rows(block_skip, device_count, GATHER_X_LAST)
        part_qkv = scatter_rows(block_qkv, device_count, GATHER_Y_LAST)
        part_out = scatter_rows(block_out, device_count, GATHER_X_LAST)
        part_up = scatter_rows(block_up, device_count, GATHER_Y_LAST)
        part_down = scatter_rows(block_down, device_count, GATHER_X_LAST)
        small_sums = sum_everywhere(small, device_count)
    grad_gains, grad_biases = small_sums[:2], small_sums[2:]
    return (
        layer_out,
        grad_in,
        grad_skip,
        part_skip,
        part_qkv,
        part_out,
        part_up,
        part_down,
        grad_gains,
        grad_biases,
    )


def solution(mesh):
    placed = (
        P(("dp", "sub"), None, None),
        P(("dp", "sub"), None, None),
        P(("dp", "sub")),
        P(("dp", "sub"), None, None),
        P(("dp", "sub")),
        P(("dp", "sub")),
        P(("dp", "sub")),
        P(("dp", "sub")),
        P(("dp", "sub")),
        P(),
        P(),
    )
    mesh_sizes = (mesh.shape["dp"], mesh.shape["sub"])
    return jax.shard_map(
        functools.partial(on_device, mesh_sizes),
        mesh=mesh,
        in_specs=placed,
        out_specs=(
            P(("dp", "sub"), None, None),
            P(("dp", "sub"), None, None),
            P(("dp", "sub"), None, None),
            P(("dp", "sub")),
            P(("dp", "sub")),
            P(("dp", "sub")),
            P(("dp", "sub")),
            P(("dp", "sub")),
            P(),
            P(),
        ),
        check_vma=False,
    )
```
